768 devices in a mesh: grp: 24 (over z_hi, y), shard: 32 (over x, z_lo, core).
Axes of the slice: x: 4, y: 8, z: 12 (z_hi: 3, z_lo: 4; z = z_hi * 4 + z_lo), core: 2. Of those that a mesh axis runs over, the one named last changes fastest.
Arguments:
- bottom_out: bfloat16 [98304, 128], P(('grp', 'shard')), may hold values from -6 to 6
- lookups: int32 [98304, 1, 4], P(('grp', 'shard')), may hold values from 0 to 251903, as said below
- starts: int32 [24, 768], replicated, may hold values from 0 to 327
- tables: float32 [1, 251904, 128], P(None, 'shard'), may hold values from -0.3 to 0.3
- top_dense: bfloat16 [128, 1024], replicated, may hold values from -0.5 to 0.5
- top_pairs: float32 [1, 1024], replicated, may hold values from -6 to 6
- cotangent: float32 [98304, 1024], P(('grp', 'shard')), may hold values from -1.5 to 1.5
Outputs:
- activation: bfloat16 [98304, 1024], P(('grp', 'shard'))
- bottom_grad: float32 [98304, 128], P(('grp', 'shard'))
- table_grad: float32 [1, 32, 7872, 128], P(None, 'shard', 'grp')
The draws below stay inside these ranges and needn't reach their ends.
Inputs may be any that keep to these rules, and one draw needn't show every extreme that they name: lookups % 328 is below 64, and 63 occurs.
All inputs are finite; a program needn't handle non-finite values.
Results may differ from the reference program's by a relative error of at most 0.0023.
Values sent between devices are 32-bit elements; how exact they have to be, the bound alone decides.
A program may use at most 32 MiB of HBM per device.

```python
import jax
import jax.numpy as jnp
from jax import lax

D = 128
HIDDEN_SIZE = 1024
ROWS_DEV = 7872
NT = 1
BAG = 4
HOT = 64
B_DEV = 128
ROWS = 251904
WIN = 328
WINDOWS = 768
BATCH = 98304
PAIRS = 1
N_GRP = 24
N_SHARD = 32


def draw_lookups(key, part):
    first_key = jax.random.fold_in(key, 11)
    second_key = jax.random.fold_in(key, 23)
    window = jax.random.randint(first_key, (BATCH, NT, BAG), 0, WINDOWS, dtype=jnp.int32)
    inner = jax.random.randint(second_key, (BATCH, NT, BAG), 0, HOT, dtype=jnp.int32)
    return (window * WIN + inner).astype(jnp.int32)


def touch_ends(values, stream_key, least, top_value):
    spot = [jax.random.randint(jax.random.fold_in(stream_key, axis), (), 0, length) for axis, length in enumerate(values.shape)]
    widest = values.shape.index(max(values.shape))
    next_to = spot[:widest] + [(spot[widest] + 1) % values.shape[widest]] + spot[widest + 1:]
    return values.at[tuple(spot)].set(least).at[tuple(next_to)].set(top_value)


def levels(key, shape, shards, low, largest):
    def one(position, shards_of):
        draws = jax.random.uniform(jax.random.fold_in(jax.random.fold_in(key, 6), position), (shards_of,), jnp.float32, low / len(shards), largest / len(shards))
        return jnp.repeat(jnp.exp(draws), shape[position] // shards_of).reshape((-1,) + (1,) * (len(shape) - position - 1))

    loudness = one(*shards[0])
    for cut in shards[1:]:
        loudness = loudness * one(*cut)
    return loudness


def normal_values(own_key, dims, spread, most, cuts=(), held_as=jnp.bfloat16):
    values = jax.random.normal(own_key, dims, jnp.float32) * spread
    if len(cuts) > 0:
        values = levels(own_key, dims, cuts, -0.22, 0.18) * values
    return jnp.clip(values, min=-most, max=most).astype(held_as)


def setup_inputs(seed: int = 0) -> dict:
    key_list = jax.random.split(jax.random.key(seed), 8)
    return {
        "bottom_out": normal_values(key_list[0], (BATCH, D), 1.0, 6.0, ((0, 768),)),
        "lookups": draw_lookups(jax.random.fold_in(key_list[7], 71), 0),
        "starts": touch_ends(jax.random.randint(key_list[2], (N_GRP, WINDOWS), 0, WIN), jax.random.fold_in(key_list[2], 1), 0, WIN - 1).astype(jnp.int32),
        "tables": normal_values(key_list[3], (NT, ROWS, D), 0.05, 0.3, ((1, 32),), jnp.float32),
        "top_dense": normal_values(key_list[4], (D, HIDDEN_SIZE), D ** -0.5, 0.5),
        "top_pairs": normal_values(key_list[5], (PAIRS, HIDDEN_SIZE), PAIRS ** -0.5, 6.0, (), jnp.float32),
        "cotangent": normal_values(key_list[6], (BATCH, HIDDEN_SIZE), 0.25, 1.5, ((0, 768),), jnp.float32),
    }


def pair_list(number):
    return [(former, latter) for former in range(number) for latter in range(former + 1, number)]


def reference(bottom_out, lookups, starts, tables, top_dense, top_pairs, cotangent):
    group_of = (jnp.arange(BATCH, dtype=jnp.int32) // (B_DEV * N_SHARD)).astype(jnp.int32)
    window = (lookups // WIN).astype(jnp.int32)
    inner = (lookups % WIN).astype(jnp.int32)
    shift = starts[group_of[:, None, None], window]
    rows = (window * WIN + (inner + shift) % WIN).astype(jnp.int32)
    pooled_list = []
    for table_pos in range(NT):
        running = jnp.zeros((BATCH, D), jnp.float32)
        for slot in range(BAG):
            running = running + tables[table_pos][rows[:, table_pos, slot]]
        pooled_list.append(running)
    vectors = [bottom_out.astype(jnp.float32)] + pooled_list
    couples = pair_list(NT + 1)
    pair_dots = jnp.stack([jnp.sum(vectors[former] * vectors[latter], axis=-1) for former, latter in couples], axis=1)
    preact = jnp.dot(bottom_out, top_dense, preferred_element_type=jnp.float32)
    preact = preact + jnp.dot(pair_dots, top_pairs, precision=lax.Precision.HIGHEST)
    sigmoid_pre = jax.nn.sigmoid(preact)
    activation = (preact * sigmoid_pre).astype(jnp.bfloat16)
    pre_grad = cotangent * sigmoid_pre * (1.0 + preact * (1.0 - sigmoid_pre))
    pair_grad = jnp.dot(pre_grad, top_pairs.T, precision=lax.Precision.HIGHEST)
    vec_grads = [jnp.zeros_like(vector) for vector in vectors]
    for place, (former, latter) in enumerate(couples):
        weight_col = pair_grad[:, place:place + 1]
        vec_grads[former] = vec_grads[former] + weight_col * vectors[latter]
        vec_grads[latter] = vec_grads[latter] + weight_col * vectors[former]
    pre_half = pre_grad.astype(jnp.bfloat16)
    bottom_grad = jnp.dot(pre_half, top_dense.T, preferred_element_type=jnp.float32) + vec_grads[0]
    grad_list = []
    for table_pos in range(NT):
        running = jnp.zeros((ROWS, D), jnp.float32)
        for slot in range(BAG):
            running = running.at[rows[:, table_pos, slot]].add(vec_grads[table_pos + 1])
        grad_list.append(running)
    table_grad = jnp.stack(grad_list, axis=0).reshape(NT, N_SHARD, ROWS_DEV, D)
    return activation, bottom_grad, table_grad
```

```python
import jax
import jax.numpy as jnp
from jax import lax
from jax.experimental import pallas as pl
from jax.experimental.pallas import tpu as pltpu
from jax.sharding import PartitionSpec as P

HOT = 64
WIN = 328
NX, NZ, NC = 4, 4, 2
ZH, NY = 3, 8
CHIPS = NX * NZ
GROUPS = ZH * NY
B = 128
D = 128
OWN = GROUPS * HOT
ROWS = NC * OWN
PAD = WIN + HOT
OUT_ROWS = 336
F32, BF16, I32 = jnp.float32, jnp.bfloat16, jnp.int32
MESH = pl.DeviceIdType.MESH


def split_bf16(value):
    high = value.astype(BF16)
    return high, (value - high.astype(F32)).astype(BF16)


def kernel(
    starts_ref, idx_ref, places_ref, v0_ref, dense_ref, pairs_ref, cot_ref, tables_ref,
    act_ref, bgrad_ref, tgrad_ref,
    win, hot, hot_t, idxs, et, part, rx, qz, zr, vs, pgs, grads, pre_dense, lsend, lrecv, outb, grecv, place_hot,
    local_sem, hot_sem, idx_send, idx_recv, vz_send, vz_recv, vx_send, vx_recv,
    rs_send, rs_recv, z_send, z_recv, pg_send, pg_recv, l_send, l_recv, g_send, g_recv,
):
    g = lax.axis_index("grp")
    s = lax.axis_index("shard")
    zh, y = g // NY, g % NY
    c = s % NC
    chip = s // NC
    x, z = chip // NZ, chip % NZ

    def at(chip_to):
        return (g, chip_to * NC + c)

    right = at((x + 1) % NX * NZ + z)
    left = at((x + NX - 1) % NX * NZ + z)
    partner = (g, chip * NC + (1 - c))

    def remote(src, dst, send, recv, to):
        return pltpu.make_async_remote_copy(
            src_ref=src, dst_ref=dst, send_sem=send, recv_sem=recv, device_id=to, device_id_type=MESH
        )

    whole = pltpu.make_async_copy(tables_ref, win.at[:, pl.ds(0, WIN)], local_sem.at[0])
    again = pltpu.make_async_copy(tables_ref.at[:, pl.ds(0, HOT)], win.at[:, pl.ds(WIN, HOT)], local_sem.at[1])
    whole.start()
    again.start()

    barrier = pltpu.get_barrier_semaphore()
    pl.semaphore_signal(barrier, inc=1, device_id=partner, device_id_type=MESH)
    for o in range(1, CHIPS):
        pl.semaphore_signal(barrier, inc=1, device_id=at((chip + o) % CHIPS), device_id_type=MESH)
    for o in range(1, GROUPS):
        pl.semaphore_signal(barrier, inc=1, device_id=((g + o) % GROUPS, s), device_id_type=MESH)
    pl.semaphore_wait(barrier, 1 + CHIPS - 1 + GROUPS - 1)

    idx_out = [
        remote(idx_ref, idxs.at[chip], idx_send.at[o - 1], idx_recv.at[chip], at((chip + o) % CHIPS))
        for o in range(1, CHIPS)
    ]
    for copy in idx_out:
        copy.start()
    vz_out = [
        remote(v0_ref, vs.at[x, z], vz_send.at[o - 1], vz_recv.at[z], at(x * NZ + (z + o) % NZ))
        for o in range(1, NZ)
    ]
    for copy in vz_out:
        copy.start()
    idxs[chip] = idx_ref[...]
    vs[x, z] = v0_ref[...]

    whole.wait()
    again.wait()
    for w in range(GROUPS):
        hot[pl.ds(c * OWN + w * HOT, HOT)] = win[w, pl.ds(starts_ref[w], HOT), :]
    mine = hot.at[pl.ds(c * OWN, OWN)]
    hot_out = remote(mine, mine, hot_sem.at[0], hot_sem.at[1], partner)
    hot_out.start()

    def turn_hot(half):
        def step(i, carry):
            at_row = pl.multiple_of(half * OWN + i * 128, 128)
            tile = hot[pl.ds(at_row, 128), :].T
            high, low = split_bf16(tile)
            hot_t[0:D, pl.ds(at_row, 128)] = high
            hot_t[D:, pl.ds(at_row, 128)] = low
            return carry

        lax.fori_loop(0, OWN // 128, step, 0, unroll=4)

    turn_hot(c)
    pre_dense[...] = jnp.dot(v0_ref[...].astype(BF16), dense_ref[...], preferred_element_type=F32)
    for o in range(1, CHIPS):
        k = (chip + o) % CHIPS
        remote(idx_ref, idxs.at[k], idx_send.at[o - 1], idx_recv.at[k], left).wait_recv()
    hot_out.wait_recv()
    turn_hot(1 - c)

    row_iota = lax.broadcasted_iota(I32, (256, B), 0).astype(F32).astype(BF16)

    rs_to = {0: right, 1: left, 2: left, 3: right, 6: right, 7: left}
    rs_slot = {0: 0, 1: 1, 2: 2, 3: 3, 6: 4, 7: 5}
    rs_out = {
        p: remote(part.at[p], rx.at[rs_slot[p]], rs_send.at[rs_slot[p]], rs_recv.at[rs_slot[p]], rs_to[p])
        for p in rs_slot
    }

    def pool_step(p, carry):
        h, q = p // 2, p % 2
        xx = (x + 2 + h * (1 + 2 * q)) % NX
        for b in range(2):
            rows = idxs[xx * NZ + 2 * q + b]
            local = rows[0:4] - chip * ROWS
            counts = rows[4:8].astype(F32).astype(BF16)
            many = [jnp.broadcast_to(counts[k : k + 1], (256, B)) for k in range(4)]

            def build(j, carry):
                near = jnp.clip(local - j * 256, -1, 256).astype(F32).astype(BF16)
                tile = jnp.zeros((256, B), BF16)
                for k in range(4):
                    tile = jnp.where(row_iota == near[k : k + 1], many[k], tile)
                et[pl.ds(pl.multiple_of(j * 256, 256), 256), pl.ds(pl.multiple_of(p * 256 + b * B, B), B)] = tile
                return carry

            lax.fori_loop(0, ROWS // 256, build, 0, unroll=2)
        both = jnp.dot(
            hot_t[...], et[:, pl.ds(pl.multiple_of(p * 256, 256), 256)], preferred_element_type=F32
        )
        summed = both[0:D] + both[D:]
        part[p, 0] = summed[:, 0:B]
        part[p, 1] = summed[:, B:]
        for k in rs_out:

            @pl.when(p == k)
            def _():
                if k >= 6:
                    rs_out[k - 6].wait_recv()
                    part[k] = part[k] + rx[k - 6]
                rs_out[k].start()

        return carry

    lax.fori_loop(0, 8, pool_step, 0)

    for o in range(1, NZ):
        k = (z + o) % NZ
        remote(v0_ref, vs.at[x, k], vz_send.at[o - 1], vz_recv.at[k], left).wait_recv()
    v_right = remote(vs.at[x], vs.at[x], vx_send.at[0], vx_recv.at[0], right)
    v_left = remote(vs.at[x], vs.at[x], vx_send.at[1], vx_recv.at[1], left)
    v_right.start()
    v_left.start()

    for q in range(2):
        a, b = (2, 4) if q == 0 else (3, 5)
        src = {2: 2, 4: 6, 3: 3, 5: 7}
        rs_out[src[a]].wait_recv()
        rs_out[src[b]].wait_recv()
        qz[pl.ds(2 * q, 2)] = part[4 + q] + rx[a] + rx[b]
    z_out = [
        remote(qz.at[(z + o) % NZ], zr.at[z], z_send.at[o - 1], z_recv.at[z], at(x * NZ + (z + o) % NZ))
        for o in range(1, NZ)
    ]
    for copy in z_out:
        copy.start()

    xl, xr = (x + NX - 1) % NX, (x + 1) % NX
    v_right.wait_recv()
    on_right = remote(vs.at[xl, pl.ds(0, 2)], vs.at[xl, pl.ds(0, 2)], vx_send.at[2], vx_recv.at[2], right)
    on_right.start()
    v_left.wait_recv()
    on_left = remote(vs.at[xr, pl.ds(2, 2)], vs.at[xr, pl.ds(2, 2)], vx_send.at[3], vx_recv.at[3], left)
    on_left.start()

    place_iota = lax.broadcasted_iota(I32, (OUT_ROWS, B), 0)
    for i in range(OWN // B):
        hit = place_iota == places_ref[:, i * B : (i + 1) * B]
        place_hot[:, i * B : (i + 1) * B] = jnp.where(hit, 1.0, 0.0).astype(BF16)

    pooled_t = qz[z]
    for o in range(1, NZ):
        k = (z + o) % NZ
        remote(qz.at[k], zr.at[k], z_send.at[o - 1], z_recv.at[k], left).wait_recv()
        pooled_t = pooled_t + zr[k]
    pooled = pooled_t.T

    v0 = v0_ref[...]
    pair_dots = jnp.sum(v0 * pooled, axis=1, keepdims=True)
    preact = pre_dense[...] + pair_dots * pairs_ref[...]
    gate = jax.nn.sigmoid(preact)
    pre_grad = cot_ref[...] * gate * (1.0 + preact * (1.0 - gate))
    pair_grad = jnp.sum(pre_grad * pairs_ref[...], axis=1, keepdims=True)
    pgs[chip] = jnp.broadcast_to(pair_grad, (B, B)).T[0:8]
    pg_out = [
        remote(pgs.at[chip], pgs.at[chip], pg_send.at[o - 1], pg_recv.at[chip], at((chip + o) % CHIPS))
        for o in range(1, CHIPS)
    ]
    for copy in pg_out:
        copy.start()
    act_ref[...] = (preact * gate).astype(BF16)
    bgrad_ref[...] = (
        lax.dot_general(
            pre_grad.astype(BF16), dense_ref[...], (((1,), (1,)), ((), ())), preferred_element_type=F32
        )
        + pair_grad * pooled
    )

    on_right.wait_recv()
    on_left.wait_recv()
    for o in range(1, CHIPS):
        k = (chip + o) % CHIPS
        remote(pgs.at[k], pgs.at[k], pg_send.at[o - 1], pg_recv.at[k], left).wait_recv()
    columns = pgs[...].reshape(CHIPS * 8, B).T
    for i in range(CHIPS):
        xi, zi = i // NZ, i % NZ
        q = zi // 2
        h = ((xi - x + 2 + NX) * (1 + 2 * q)) % 4
        row = pl.multiple_of((2 * h + q) * 256 + (zi % 2) * B, B)
        high, low = split_bf16(vs[xi, zi] * columns[:, 8 * i : 8 * i + 1])
        grads[pl.ds(row, B), 0:D] = high
        grads[pl.ds(row, B), D:] = low

    def row_grads(half, t):
        row = pl.multiple_of(half * OWN + t * NY * HOT, NY * HOT)
        both = jnp.dot(et[pl.ds(row, NY * HOT), :], grads[...], preferred_element_type=F32)
        return both[:, 0:D] + both[:, D:]

    l_out = [remote(lsend.at[i], lrecv.at[i], l_send.at[i], l_recv.at[i], partner) for i in range(ZH)]
    for i in range(ZH):
        lsend[i] = row_grads(1 - c, (zh + 1 + i) % ZH)
        l_out[i].start()
    g_out = []
    for i in range(ZH):
        t = (zh + 1 + i) % ZH
        total = row_grads(c, t)
        l_out[i].wait_recv()
        outb[i] = (total + lrecv[i]).reshape(NY, HOT, D)
        for o in range(1, NY + 1):
            k = (y + o) % NY
            if i == ZH - 1 and o == NY:
                continue
            copy = remote(outb.at[i, k], grecv.at[g], g_send.at[len(g_out)], g_recv.at[g], (t * NY + k, s))
            copy.start()
            g_out.append(copy)
    grecv[g] = outb[ZH - 1, y]
    for o in range(1, GROUPS):
        k = (g + o) % GROUPS
        remote(grecv.at[k], grecv.at[k], g_send.at[o - 1], g_recv.at[k], left).wait_recv()
    high, low = split_bf16(grecv[...].reshape(OWN, D))
    both = jnp.dot(place_hot[...], jnp.concatenate([high, low], axis=1), preferred_element_type=F32)
    tgrad_ref[...] = (both[:, 0:D] + both[:, D:])[0:WIN]

    hot_out.wait_send()
    for copy in (*idx_out, *vz_out, *rs_out.values(), v_right, v_left, on_right, on_left):
        copy.wait_send()
    for copy in (*z_out, *pg_out, *l_out, *g_out):
        copy.wait_send()


def on_device(bottom_out, lookups, starts, tables, top_dense, top_pairs, cotangent):
    g = lax.axis_index("grp")
    s = lax.axis_index("shard")
    picked = lookups[:, 0, :].T
    hot_index = picked // WIN * HOT + picked % WIN
    counts = jnp.sum((hot_index[:, None, :] == hot_index[None, :, :]).astype(I32), axis=1)
    idx = jnp.concatenate([hot_index, counts], axis=0)
    my_starts = lax.dynamic_slice(starts, (g, s * GROUPS), (1, GROUPS))[0]
    recv_starts = lax.dynamic_slice(starts, (0, s * GROUPS + g), (GROUPS, 1))
    places = ((recv_starts + jnp.arange(HOT, dtype=I32)[None, :]) % WIN).reshape(1, OWN)
    vmem = pl.BlockSpec(memory_space=pltpu.VMEM)
    dma = pltpu.SemaphoreType.DMA
    act, bgrad, tgrad = pl.pallas_call(
        kernel,
        out_shape=(
            jax.ShapeDtypeStruct((B, 1024), BF16),
            jax.ShapeDtypeStruct((B, D), F32),
            jax.ShapeDtypeStruct((WIN, D), F32),
        ),
        in_specs=[pl.BlockSpec(memory_space=pltpu.SMEM)] + [vmem] * 6 + [pl.BlockSpec(memory_space=pl.ANY)],
        out_specs=(vmem, vmem, vmem),
        scratch_shapes=[
            pltpu.VMEM((GROUPS, PAD, D), F32),
            pltpu.VMEM((ROWS, D), F32),
            pltpu.VMEM((2 * D, ROWS), BF16),
            pltpu.VMEM((CHIPS, 8, B), I32),
            pltpu.VMEM((ROWS, CHIPS * B), BF16),
            pltpu.VMEM((8, 2, D, B), F32),
            pltpu.VMEM((6, 2, D, B), F32),
            pltpu.VMEM((NZ, D, B), F32),
            pltpu.VMEM((NZ, D, B), F32),
            pltpu.VMEM((NX, NZ, B, D), F32),
            pltpu.VMEM((CHIPS, 8, B), F32),
            pltpu.VMEM((CHIPS * B, 2 * D), BF16),
            pltpu.VMEM((B, 1024), F32),
            pltpu.VMEM((ZH, NY * HOT, D), F32),
            pltpu.VMEM((ZH, NY * HOT, D), F32),
            pltpu.VMEM((ZH, NY, HOT, D), F32),
            pltpu.VMEM((GROUPS, HOT, D), F32),
            pltpu.VMEM((OUT_ROWS, OWN), BF16),
            dma((2,)), dma((2,)), dma((CHIPS - 1,)), dma((CHIPS,)), dma((NZ - 1,)), dma((NZ,)), dma((4,)), dma((4,)),
            dma((6,)), dma((6,)), dma((NZ - 1,)), dma((NZ,)), dma((CHIPS - 1,)), dma((CHIPS,)),
            dma((ZH,)), dma((ZH,)), dma((GROUPS - 1,)), dma((GROUPS,)),
        ],
        compiler_params=pltpu.CompilerParams(
            collective_id=0, has_side_effects=True, vmem_limit_bytes=60 * 1024 * 1024
        ),
    )(
        my_starts, idx, places, bottom_out.astype(F32), top_dense, top_pairs, cotangent,
        tables.reshape(GROUPS, WIN, D),
    )
    return act, bgrad, tgrad[None, None]


def solution(mesh):
    in_specs = (
        P(("grp", "shard"), None),
        P(("grp", "shard"), None, None),
        P(),
        P(None, "shard", None),
        P(),
        P(),
        P(("grp", "shard"), None),
    )
    out_specs = (
        P(("grp", "shard"), None),
        P(("grp", "shard"), None),
        P(None, "shard", "grp", None),
    )
    return jax.shard_map(
        on_device, mesh=mesh, in_specs=in_specs, out_specs=out_specs, check_vma=False
    )
```

```python
import jax
import jax.numpy as jnp
from jax import lax
from jax.experimental import pallas as pl
from jax.experimental.pallas import tpu as pltpu
from jax.sharding import PartitionSpec as P

HOT = 64
WIN = 328
NX, NZ, NC = 4, 4, 2
ZH, NY = 3, 8
CHIPS = NX * NZ
GROUPS = ZH * NY
B = 128
D = 128
OWN = GROUPS * HOT
ROWS = NC * OWN
PAD = WIN + HOT
OUT_ROWS = 336
F32, BF16, I32 = jnp.float32, jnp.bfloat16, jnp.int32
MESH = pl.DeviceIdType.MESH


def split_bf16(value):
    high = value.astype(BF16)
    return high, (value - high.astype(F32)).astype(BF16)


def kernel(
    bottom_hbm, lookups_hbm, pairs_hbm, starts_ref, tables_ref, dense_hbm, cot_hbm,
    act_ref, bgrad_ref, tgrad_ref,
    bottom_ref, lookups_ref, pairs_ref, dense_ref, cot_ref, start_of, win, hot, hot_t, idxs, et_a, et_b, part, rx, qz, zr, vs, pgs, grads, pre_dense, lsend, lrecv, outb, grecv, place_hot,
    local_sem, hot_sem, idx_send, idx_recv, vz_send, vz_recv, vx_send, vx_recv,
    rs_send, rs_recv, z_send, z_recv, pg_send, pg_recv, l_send, l_recv, g_send, g_recv,
):
    g = lax.axis_index("grp")
    s = lax.axis_index("shard")
    zh, y = g // NY, g % NY
    et = (et_a, et_b)
    c = s % NC
    chip = s // NC
    x, z = chip // NZ, chip % NZ

    def at(chip_to):
        return (g, chip_to * NC + c)

    right = at((x + 1) % NX * NZ + z)
    left = at((x + NX - 1) % NX * NZ + z)
    partner = (g, chip * NC + (1 - c))

    def remote(src, dst, send, recv, to):
        return pltpu.make_async_remote_copy(
            src_ref=src, dst_ref=dst, send_sem=send, recv_sem=recv, device_id=to, device_id_type=MESH
        )

    first = (s * GROUPS // 128 - s // 27) * 128
    starts_in = pltpu.make_async_copy(starts_ref.at[:, pl.ds(pl.multiple_of(first, 128), 256)], start_of, local_sem.at[2])
    whole = pltpu.make_async_copy(tables_ref, win.at[:, pl.ds(0, WIN)], local_sem.at[0])
    again = pltpu.make_async_copy(tables_ref.at[:, pl.ds(0, HOT)], win.at[:, pl.ds(WIN, HOT)], local_sem.at[1])
    dense_in = pltpu.make_async_copy(dense_hbm, dense_ref, local_sem.at[3])
    cot_in = pltpu.make_async_copy(cot_hbm, cot_ref, local_sem.at[4])
    lookups_in = pltpu.make_async_copy(lookups_hbm, lookups_ref, local_sem.at[5])
    bottom_in = pltpu.make_async_copy(bottom_hbm, bottom_ref, local_sem.at[6])
    pairs_in = pltpu.make_async_copy(pairs_hbm, pairs_ref, local_sem.at[7])
    for copy in (lookups_in, bottom_in, starts_in, whole, again, dense_in, cot_in, pairs_in):
        copy.start()

    barrier = pltpu.get_barrier_semaphore()
    pl.semaphore_signal(barrier, inc=1, device_id=partner, device_id_type=MESH)
    for o in range(1, CHIPS):
        pl.semaphore_signal(barrier, inc=1, device_id=at((chip + o) % CHIPS), device_id_type=MESH)
    for o in range(1, GROUPS):
        pl.semaphore_signal(barrier, inc=1, device_id=((g + o) % GROUPS, s), device_id_type=MESH)

    lookups_in.wait()
    picked = lookups_ref[...]
    window = ((picked.astype(F32) + 0.5) * (1.0 / WIN)).astype(I32)
    hot_index = picked - window * (WIN - HOT)
    counts = jnp.zeros((4, B), I32)
    for k in range(4):
        counts = counts + jnp.where(hot_index == hot_index[k : k + 1], 1, 0)
    idxs[chip, 0:4] = hot_index
    idxs[chip, 4:8] = counts
    bottom_in.wait()
    vs[x, z] = bottom_ref[...].astype(F32)
    starts_in.wait()
    whole.wait()
    again.wait()
    for w in range(GROUPS):
        hot[pl.ds(c * OWN + w * HOT, HOT)] = win[w, pl.ds(start_of[g, s * GROUPS - first + w], HOT), :]
    pl.semaphore_wait(barrier, 1 + CHIPS - 1 + GROUPS - 1)

    idx_out = [
        remote(idxs.at[chip], idxs.at[chip], idx_send.at[o - 1], idx_recv.at[chip], at((chip + o) % CHIPS))
        for o in range(1, CHIPS)
    ]
    for copy in idx_out:
        copy.start()
    mine = hot.at[pl.ds(c * OWN, OWN)]
    hot_out = remote(mine, mine, hot_sem.at[0], hot_sem.at[1], partner)
    hot_out.start()
    vz_out = [
        remote(vs.at[x, z], vs.at[x, z], vz_send.at[o - 1], vz_recv.at[z], at(x * NZ + (z + o) % NZ))
        for o in range(1, NZ)
    ]
    for copy in vz_out:
        copy.start()

    def turn_hot(half):
        def step(i, carry):
            at_row = pl.multiple_of(half * OWN + i * 128, 128)
            tile = hot[pl.ds(at_row, 128), :].T
            high, low = split_bf16(tile)
            hot_t[half * GROUPS // 2 + i, 0:D] = high
            hot_t[half * GROUPS // 2 + i, D:] = low
            return carry

        lax.fori_loop(0, OWN // 128, step, 0, unroll=4)

    turn_hot(c)
    dense_in.wait()
    pre_dense[...] = jnp.dot(bottom_ref[...], dense_ref[...], preferred_element_type=F32)
    for o in range(1, CHIPS):
        k = (chip + o) % CHIPS
        remote(idxs.at[k], idxs.at[k], idx_send.at[o - 1], idx_recv.at[k], left).wait_recv()
    hot_out.wait_recv()
    turn_hot(1 - c)

    row_iota = lax.broadcasted_iota(I32, (256, B), 0).astype(F32).astype(BF16)

    rs_to = {0: right, 1: left, 2: left, 3: right, 6: right, 7: left}
    rs_slot = {0: 0, 1: 1, 2: 2, 3: 3, 6: 4, 7: 5}
    rs_out = {
        p: remote(part.at[p], rx.at[rs_slot[p]], rs_send.at[rs_slot[p]], rs_recv.at[rs_slot[p]], rs_to[p])
        for p in rs_slot
    }

    def build(h, q):
        xx = (x + 2 + h * (1 + 2 * q)) % NX
        for b in range(2):
            rows = idxs[xx * NZ + 2 * q + b]
            local = rows[0:4] - chip * ROWS
            counts = rows[4:8].astype(F32).astype(BF16)
            for j in range(ROWS // 256):
                near = jnp.clip(local - j * 256, -1, 256).astype(F32).astype(BF16)
                tile = jnp.zeros((256, B), BF16)
                for k in range(4):
                    tile = jnp.where(row_iota == near[k : k + 1], counts[k : k + 1], tile)
                et[q][2 * h + b, j] = tile

    def pool(h, q):
        both = jnp.dot(
            jnp.concatenate([hot_t[i] for i in range(ROWS // 128)], axis=1),
            jnp.concatenate([et[q][2 * h + b].reshape(ROWS, B) for b in range(2)], axis=1),
            preferred_element_type=F32,
        )
        summed = both[0:D] + both[D:]
        part[2 * h + q, 0] = summed[:, 0:B]
        part[2 * h + q, 1] = summed[:, B:]

    def pass_on(h, q):
        for k in rs_out:
            if k % 2 == q:

                @pl.when(h == k // 2)
                def _():
                    if k >= 6:
                        rs_out[k - 6].wait_recv()
                        part[k] = part[k] + rx[k - 6]
                    rs_out[k].start()

    build(0, 0)

    def pool_step(h, carry):
        build(h, 1)
        pool(h, 0)
        pass_on(h, 0)
        build((h + 1) % 4, 0)
        pool(h, 1)
        pass_on(h, 1)
        return carry

    lax.fori_loop(0, 4, pool_step, 0)

    for o in range(1, NZ):
        k = (z + o) % NZ
        remote(vs.at[x, k], vs.at[x, k], vz_send.at[o - 1], vz_recv.at[k], left).wait_recv()
    v_right = remote(vs.at[x], vs.at[x], vx_send.at[0], vx_recv.at[0], right)
    v_left = remote(vs.at[x], vs.at[x], vx_send.at[1], vx_recv.at[1], left)
    v_right.start()
    v_left.start()

    for q in range(2):
        a, b = (2, 4) if q == 0 else (3, 5)
        src = {2: 2, 4: 6, 3: 3, 5: 7}
        rs_out[src[a]].wait_recv()
        rs_out[src[b]].wait_recv()
        qz[pl.ds(2 * q, 2)] = part[4 + q] + rx[a] + rx[b]
    z_out = [
        remote(qz.at[(z + o) % NZ], zr.at[z], z_send.at[o - 1], z_recv.at[z], at(x * NZ + (z + o) % NZ))
        for o in range(1, NZ)
    ]
    for copy in z_out:
        copy.start()

    xl, xr = (x + NX - 1) % NX, (x + 1) % NX
    v_right.wait_recv()
    on_right = remote(vs.at[xl, pl.ds(0, 2)], vs.at[xl, pl.ds(0, 2)], vx_send.at[2], vx_recv.at[2], right)
    on_right.start()
    v_left.wait_recv()
    on_left = remote(vs.at[xr, pl.ds(2, 2)], vs.at[xr, pl.ds(2, 2)], vx_send.at[3], vx_recv.at[3], left)
    on_left.start()

    place_iota = lax.broadcasted_iota(I32, (OUT_ROWS, B), 0)
    lane = lax.broadcasted_iota(I32, (1, B), 1)
    column = s * GROUPS - first + g
    for i in range(OWN // B):
        place = lane % HOT + jnp.where(lane < HOT, start_of[2 * i, column], start_of[2 * i + 1, column])
        place = jnp.where(place >= WIN, place - WIN, place)
        place_hot[i] = jnp.where(place_iota == place, 1.0, 0.0).astype(BF16)

    pooled_t = qz[z]
    for o in range(1, NZ):
        k = (z + o) % NZ
        remote(qz.at[k], zr.at[k], z_send.at[o - 1], z_recv.at[k], left).wait_recv()
        pooled_t = pooled_t + zr[k]
    pooled = pooled_t.T

    v0 = bottom_ref[...].astype(F32)
    cot_in.wait()
    pairs_in.wait()
    pair_dots = jnp.sum(v0 * pooled, axis=1, keepdims=True)
    preact = pre_dense[...] + pair_dots * pairs_ref[...]
    gate = jax.nn.sigmoid(preact)
    pre_grad = cot_ref[...] * gate * (1.0 + preact * (1.0 - gate))
    pair_grad = jnp.sum(pre_grad * pairs_ref[...], axis=1, keepdims=True)
    pgs[chip] = jnp.broadcast_to(pair_grad, (B, B)).T[0:8]
    pg_out = [
        remote(pgs.at[chip], pgs.at[chip], pg_send.at[o - 1], pg_recv.at[chip], at((chip + o) % CHIPS))
        for o in range(1, CHIPS)
    ]
    for copy in pg_out:
        copy.start()
    act_ref[...] = (preact * gate).astype(BF16)
    bgrad_ref[...] = (
        lax.dot_general(
            pre_grad.astype(BF16), dense_ref[...], (((1,), (1,)), ((), ())), preferred_element_type=F32
        )
        + pair_grad * pooled
    )

    on_right.wait_recv()
    on_left.wait_recv()
    for o in range(1, CHIPS):
        k = (chip + o) % CHIPS
        remote(pgs.at[k], pgs.at[k], pg_send.at[o - 1], pg_recv.at[k], left).wait_recv()
    columns = pgs[...].reshape(CHIPS * 8, B).T
    for i in range(CHIPS):
        xi, zi = i // NZ, i % NZ
        q = zi // 2
        h = ((xi - x + 2 + NX) * (1 + 2 * q)) % 4
        slot = q * 8 + 2 * h + zi % 2
        high, low = split_bf16(vs[xi, zi] * columns[:, 8 * i : 8 * i + 1])
        grads[0, slot] = high
        grads[1, slot] = low

    half_to = y // 4

    def spans(i):
        if i == 2:
            return [(zh, 0), (zh, 1)]
        block = (half_to + 1 + i) % 2
        return [((zh + 1) % ZH, block), ((zh + 2) % ZH, block)]

    def row_grads(half, i):
        rows = [
            jnp.concatenate([et[k // 8][k % 8, half * (OWN // 256) + t * 2 + block] for k in range(CHIPS)], axis=1)
            for t, block in spans(i)
        ]
        right_side = jnp.concatenate([grads[k].reshape(CHIPS * B, D) for k in range(2)], axis=1)
        both = jnp.dot(jnp.concatenate(rows, axis=0), right_side, preferred_element_type=F32)
        return both[:, 0:D] + both[:, D:]

    l_out = [remote(lsend.at[i], lrecv.at[i], l_send.at[i], l_recv.at[i], partner) for i in range(3)]
    g_out = []
    for i in range(3):
        lsend[i] = row_grads(1 - c, i)
        l_out[i].start()
        total = row_grads(c, i)
        l_out[i].wait_recv()
        outb[i] = (total + lrecv[i]).reshape(NY, HOT, D)
        if i < 2:
            (t, block), (u, _) = spans(i)
            order = [(zz, part_of * 4 + k, block * 4 + k) for k in range(4) for part_of, zz in ((0, t), (1, u))]
        else:
            order = [(zh, (y + o) % NY, (y + o) % NY) for o in range(1, NY)]
        for zz, k, yy in order:
            copy = remote(outb.at[i, k], grecv.at[g], g_send.at[len(g_out)], g_recv.at[g], (zz * NY + yy, s))
            copy.start()
            g_out.append(copy)
    grecv[g] = outb[2, y]
    for o in range(1, GROUPS):
        k = (g + o) % GROUPS
        remote(grecv.at[k], grecv.at[k], g_send.at[o - 1], g_recv.at[k], left).wait_recv()
    high, low = split_bf16(grecv[...].reshape(OWN, D))
    both = jnp.dot(
        jnp.concatenate([place_hot[i] for i in range(OWN // B)], axis=1),
        jnp.concatenate([high, low], axis=1),
        preferred_element_type=F32,
    )
    tgrad_ref[...] = (both[:, 0:D] + both[:, D:])[0:WIN]

    hot_out.wait_send()
    for copy in (*idx_out, *vz_out, *rs_out.values(), v_right, v_left, on_right, on_left):
        copy.wait_send()
    for copy in (*z_out, *pg_out, *l_out, *g_out):
        copy.wait_send()


def keep(*refs):
    for source, target in zip(refs[:3], refs[3:]):
        target[...] = source[...]


def on_device(bottom_out, lookups, starts, tables, top_dense, top_pairs, cotangent):
    vmem = pl.BlockSpec(memory_space=pltpu.VMEM)
    dma = pltpu.SemaphoreType.DMA
    hbm = pl.BlockSpec(memory_space=pltpu.HBM)
    shapes = (
        jax.ShapeDtypeStruct((B, 1024), BF16),
        jax.ShapeDtypeStruct((B, D), F32),
        jax.ShapeDtypeStruct((WIN, D), F32),
    )
    operands = (
        bottom_out, lookups[:, 0, :].T, top_pairs, starts, tables.reshape(GROUPS, WIN, D), top_dense, cotangent,
    )
    results = pl.pallas_call(
        kernel,
        out_shape=shapes,
        in_specs=[hbm] * 7,
        out_specs=(vmem, vmem, vmem),
        scratch_shapes=[
            pltpu.VMEM((B, D), BF16),
            pltpu.VMEM((4, B), I32),
            pltpu.VMEM((1, 1024), F32),
            pltpu.VMEM((D, 1024), BF16),
            pltpu.VMEM((B, 1024), F32),
            pltpu.SMEM((GROUPS, 256), I32),
            pltpu.VMEM((GROUPS, PAD, D), F32),
            pltpu.VMEM((ROWS, D), F32),
            pltpu.VMEM((ROWS // 128, 2 * D, 128), BF16),
            pltpu.VMEM((CHIPS, 8, B), I32),
            pltpu.VMEM((CHIPS // 2, ROWS // 256, 256, B), BF16),
            pltpu.VMEM((CHIPS // 2, ROWS // 256, 256, B), BF16),
            pltpu.VMEM((8, 2, D, B), F32),
            pltpu.VMEM((6, 2, D, B), F32),
            pltpu.VMEM((NZ, D, B), F32),
            pltpu.VMEM((NZ, D, B), F32),
            pltpu.VMEM((NX, NZ, B, D), F32),
            pltpu.VMEM((CHIPS, 8, B), F32),
            pltpu.VMEM((2, CHIPS, B, D), BF16),
            pltpu.VMEM((B, 1024), F32),
            pltpu.VMEM((ZH, NY * HOT, D), F32),
            pltpu.VMEM((ZH, NY * HOT, D), F32),
            pltpu.VMEM((ZH, NY, HOT, D), F32),
            pltpu.VMEM((GROUPS, HOT, D), F32),
            pltpu.VMEM((OWN // B, OUT_ROWS, B), BF16),
            dma((8,)), dma((2,)), dma((CHIPS - 1,)), dma((CHIPS,)), dma((NZ - 1,)), dma((NZ,)), dma((4,)), dma((4,)),
            dma((6,)), dma((6,)), dma((NZ - 1,)), dma((NZ,)), dma((CHIPS - 1,)), dma((CHIPS,)),
            dma((ZH,)), dma((ZH,)), dma((GROUPS - 1,)), dma((GROUPS,)),
        ],
        compiler_params=pltpu.CompilerParams(
            collective_id=0, has_side_effects=True, vmem_limit_bytes=38 * 1024 * 1024
        ),
    )(
        *(pltpu.with_memory_space_constraint(value, pltpu.HBM) for value in operands)
    )
    act, bgrad, tgrad = pl.pallas_call(
        keep,
        out_shape=shapes,
        in_specs=[vmem] * 3,
        out_specs=(vmem,) * 3,
        compiler_params=pltpu.CompilerParams(vmem_limit_bytes=4 * 1024 * 1024),
    )(*results)
    return act, bgrad, tgrad[None, None]


def solution(mesh):
    in_specs = (
        P(("grp", "shard"), None),
        P(("grp", "shard"), None, None),
        P(),
        P(None, "shard", None),
        P(),
        P(),
        P(("grp", "shard"), None),
    )
    out_specs = (
        P(("grp", "shard"), None),
        P(("grp", "shard"), None),
        P(None, "shard", "grp", None),
    )
    return jax.shard_map(
        on_device, mesh=mesh, in_specs=in_specs, out_specs=out_specs, check_vma=False
    )
```

```python
import jax
import jax.numpy as jnp
from jax import lax
from jax.experimental import pallas as pl
from jax.experimental.pallas import tpu as pltpu
from jax.sharding import PartitionSpec as P

HOT = 64
WIN = 328
NX, NZ, NC = 4, 4, 2
ZH, NY = 3, 8
CHIPS = NX * NZ
GROUPS = ZH * NY
B = 128
D = 128
OWN = GROUPS * HOT
ROWS = NC * OWN
PAD = WIN + HOT
OUT_ROWS = 336
F32, BF16, I32 = jnp.float32, jnp.bfloat16, jnp.int32
MESH = pl.DeviceIdType.MESH


def split_bf16(value):
    high = value.astype(BF16)
    return high, (value - high.astype(F32)).astype(BF16)


def kernel(
    bottom_hbm, lookups_hbm, pairs_hbm, starts_ref, tables_ref, dense_hbm, cot_hbm,
    act_ref, bgrad_ref, tgrad_ref,
    bottom_ref, lookups_ref, pairs_ref, dense_ref, cot_ref, start_of, win, hot, hot_t, idxs, et_a, et_b, part, rx, qz, zr, vs, pgs, grads, pre_dense, lsend, lrecv, outb, grecv, place_hot,
    local_sem, hot_sem, idx_send, idx_recv, vz_send, vz_recv, vx_send, vx_recv,
    rs_send, rs_recv, z_send, z_recv, pg_send, pg_recv, l_send, l_recv, g_send, g_recv,
):
    g = lax.axis_index("grp")
    s = lax.axis_index("shard")
    zh, y = g // NY, g % NY
    et = (et_a, et_b)
    c = s % NC
    chip = s // NC
    x, z = chip // NZ, chip % NZ

    def at(chip_to):
        return (g, chip_to * NC + c)

    right = at((x + 1) % NX * NZ + z)
    left = at((x + NX - 1) % NX * NZ + z)
    partner = (g, chip * NC + (1 - c))

    def remote(src, dst, send, recv, to):
        return pltpu.make_async_remote_copy(
            src_ref=src, dst_ref=dst, send_sem=send, recv_sem=recv, device_id=to, device_id_type=MESH
        )

    first = (s * GROUPS // 128 - s // 27) * 128
    starts_in = pltpu.make_async_copy(starts_ref.at[:, pl.ds(pl.multiple_of(first, 128), 256)], start_of, local_sem.at[2])
    whole = pltpu.make_async_copy(tables_ref, win.at[:, pl.ds(0, WIN)], local_sem.at[0])
    again = pltpu.make_async_copy(tables_ref.at[:, pl.ds(0, HOT)], win.at[:, pl.ds(WIN, HOT)], local_sem.at[1])
    dense_in = pltpu.make_async_copy(dense_hbm, dense_ref, local_sem.at[3])
    cot_in = pltpu.make_async_copy(cot_hbm, cot_ref, local_sem.at[4])
    lookups_in = pltpu.make_async_copy(lookups_hbm, lookups_ref, local_sem.at[5])
    bottom_in = pltpu.make_async_copy(bottom_hbm, bottom_ref, local_sem.at[6])
    pairs_in = pltpu.make_async_copy(pairs_hbm, pairs_ref, local_sem.at[7])
    for copy in (lookups_in, bottom_in, starts_in, whole, again, dense_in, cot_in, pairs_in):
        copy.start()

    barrier = pltpu.get_barrier_semaphore()
    pl.semaphore_signal(barrier, inc=1, device_id=partner, device_id_type=MESH)
    for o in range(1, CHIPS):
        pl.semaphore_signal(barrier, inc=1, device_id=at((chip + o) % CHIPS), device_id_type=MESH)
    for o in range(1, GROUPS):
        pl.semaphore_signal(barrier, inc=1, device_id=((g + o) % GROUPS, s), device_id_type=MESH)

    lookups_in.wait()
    picked = lookups_ref[...]
    window = ((picked.astype(F32) + 0.5) * (1.0 / WIN)).astype(I32)
    hot_index = picked - window * (WIN - HOT)
    counts = jnp.zeros((4, B), I32)
    for k in range(4):
        counts = counts + jnp.where(hot_index == hot_index[k : k + 1], 1, 0)
    idxs[chip, 0:4] = hot_index
    idxs[chip, 4:8] = counts
    bottom_in.wait()
    vs[x, z] = bottom_ref[...].astype(F32)
    pl.semaphore_wait(barrier, 1 + CHIPS - 1 + GROUPS - 1)

    idx_out = [
        remote(idxs.at[chip], idxs.at[chip], idx_send.at[o - 1], idx_recv.at[chip], at((chip + o) % CHIPS))
        for o in range(1, CHIPS)
    ]
    for copy in idx_out:
        copy.start()
    starts_in.wait()
    whole.wait()
    again.wait()
    for w in range(GROUPS):
        hot[pl.ds(c * OWN + w * HOT, HOT)] = win[w, pl.ds(start_of[g, s * GROUPS - first + w], HOT), :]
    mine = hot.at[pl.ds(c * OWN, OWN)]
    hot_out = remote(mine, mine, hot_sem.at[0], hot_sem.at[1], partner)
    hot_out.start()

    def turn_hot(half):
        def step(i, carry):
            at_row = pl.multiple_of(half * OWN + i * 128, 128)
            tile = hot[pl.ds(at_row, 128), :].T
            high, low = split_bf16(tile)
            hot_t[half * GROUPS // 2 + i, 0:D] = high
            hot_t[half * GROUPS // 2 + i, D:] = low
            return carry

        lax.fori_loop(0, OWN // 128, step, 0, unroll=4)

    turn_hot(c)
    dense_in.wait()
    pre_dense[...] = jnp.dot(bottom_ref[...], dense_ref[...], preferred_element_type=F32)
    for o in range(1, CHIPS):
        k = (chip + o) % CHIPS
        remote(idxs.at[k], idxs.at[k], idx_send.at[o - 1], idx_recv.at[k], left).wait_recv()
    vz_out = [
        remote(vs.at[x, z], vs.at[x, z], vz_send.at[o - 1], vz_recv.at[z], at(x * NZ + (z + o) % NZ))
        for o in range(1, NZ)
    ]
    for copy in vz_out:
        copy.start()
    hot_out.wait_recv()
    turn_hot(1 - c)

    row_iota = lax.broadcasted_iota(I32, (256, B), 0).astype(F32).astype(BF16)

    rs_to = {0: right, 1: left, 2: left, 3: right, 4: right, 5: left}
    rs_out = {p: remote(part.at[p], rx.at[p], rs_send.at[p], rs_recv.at[p], to) for p, to in rs_to.items()}

    def x_of(h, q):
        return (x + (2 + h + h // 2 * (2 * h - 3)) * (1 + 2 * q)) % NX

    def turn_of(xx, q):
        m = ((xx - x + NX) * (1 + 2 * q) + 2) % NX
        return m + m // 2 * (5 - 2 * m)

    def build(h, q):
        xx = x_of(h, q)
        for b in range(2):
            rows = idxs[xx * NZ + 2 * q + b]
            local = rows[0:4] - chip * ROWS
            counts = rows[4:8].astype(F32).astype(BF16)
            for j in range(ROWS // 256):
                near = jnp.clip(local - j * 256, -1, 256).astype(F32).astype(BF16)
                tile = jnp.zeros((256, B), BF16)
                for k in range(4):
                    tile = jnp.where(row_iota == near[k : k + 1], counts[k : k + 1], tile)
                et[q][2 * h + b, j] = tile

    def pool(h, q):
        both = jnp.dot(
            jnp.concatenate([hot_t[i] for i in range(ROWS // 128)], axis=1),
            jnp.concatenate([et[q][2 * h + b].reshape(ROWS, B) for b in range(2)], axis=1),
            preferred_element_type=F32,
        )
        summed = both[0:D] + both[D:]
        part[2 * h + q, 0] = summed[:, 0:B]
        part[2 * h + q, 1] = summed[:, B:]

    def pass_on(h, q):
        for k in rs_out:
            if k % 2 == q:

                @pl.when(h == k // 2)
                def _():
                    if k >= 4:
                        rs_out[k - 4].wait_recv()
                        part[k] = part[k] + rx[k - 4]
                    rs_out[k].start()
                    if k == 5:
                        for o in range(1, NZ):
                            kz = (z + o) % NZ
                            remote(vs.at[x, kz], vs.at[x, kz], vz_send.at[o - 1], vz_recv.at[kz], left).wait_recv()
                        v_right.start()
                        v_left.start()

    v_right = remote(vs.at[x], vs.at[x], vx_send.at[0], vx_recv.at[0], right)
    v_left = remote(vs.at[x], vs.at[x], vx_send.at[1], vx_recv.at[1], left)

    build(0, 0)

    def pool_step(h, carry):
        build(h, 1)
        pool(h, 0)
        pass_on(h, 0)
        build((h + 1) % 4, 0)
        pool(h, 1)
        pass_on(h, 1)
        return carry

    lax.fori_loop(0, 4, pool_step, 0)

    for q in range(2):
        a, b = (2, 4) if q == 0 else (3, 5)
        rs_out[a].wait_recv()
        rs_out[b].wait_recv()
        qz[pl.ds(2 * q, 2)] = part[6 + q] + rx[a] + rx[b]
    z_out = [
        remote(qz.at[(z + o) % NZ], zr.at[z], z_send.at[o - 1], z_recv.at[z], at(x * NZ + (z + o) % NZ))
        for o in range(1, NZ)
    ]
    for copy in z_out:
        copy.start()

    xl, xr = (x + NX - 1) % NX, (x + 1) % NX
    v_right.wait_recv()
    on_right = remote(vs.at[xl, pl.ds(0, 2)], vs.at[xl, pl.ds(0, 2)], vx_send.at[2], vx_recv.at[2], right)
    on_right.start()
    v_left.wait_recv()
    on_left = remote(vs.at[xr, pl.ds(2, 2)], vs.at[xr, pl.ds(2, 2)], vx_send.at[3], vx_recv.at[3], left)
    on_left.start()

    place_iota = lax.broadcasted_iota(I32, (OUT_ROWS, B), 0)
    lane = lax.broadcasted_iota(I32, (1, B), 1)
    column = s * GROUPS - first + g
    for i in range(OWN // B):
        place = lane % HOT + jnp.where(lane < HOT, start_of[2 * i, column], start_of[2 * i + 1, column])
        place = jnp.where(place >= WIN, place - WIN, place)
        place_hot[i] = jnp.where(place_iota == place, 1.0, 0.0).astype(BF16)

    pooled_t = qz[z]
    for o in range(1, NZ):
        k = (z + o) % NZ
        remote(qz.at[k], zr.at[k], z_send.at[o - 1], z_recv.at[k], left).wait_recv()
        pooled_t = pooled_t + zr[k]
    pooled = pooled_t.T

    v0 = bottom_ref[...].astype(F32)
    cot_in.wait()
    pairs_in.wait()
    pair_dots = jnp.sum(v0 * pooled, axis=1, keepdims=True)
    preact = pre_dense[...] + pair_dots * pairs_ref[...]
    gate = jax.nn.sigmoid(preact)
    pre_grad = cot_ref[...] * gate * (1.0 + preact * (1.0 - gate))
    pair_grad = jnp.sum(pre_grad * pairs_ref[...], axis=1, keepdims=True)
    pgs[chip] = jnp.broadcast_to(pair_grad, (B, B)).T[0:8]
    pg_out = [
        remote(pgs.at[chip], pgs.at[chip], pg_send.at[o - 1], pg_recv.at[chip], at((chip + o) % CHIPS))
        for o in range(1, CHIPS)
    ]
    for copy in pg_out:
        copy.start()
    act_ref[...] = (preact * gate).astype(BF16)
    bgrad_ref[...] = (
        lax.dot_general(
            pre_grad.astype(BF16), dense_ref[...], (((1,), (1,)), ((), ())), preferred_element_type=F32
        )
        + pair_grad * pooled
    )

    on_right.wait_recv()
    on_left.wait_recv()
    for o in range(1, CHIPS):
        k = (chip + o) % CHIPS
        remote(pgs.at[k], pgs.at[k], pg_send.at[o - 1], pg_recv.at[k], left).wait_recv()
    columns = pgs[...].reshape(CHIPS * 8, B).T
    for i in range(CHIPS):
        xi, zi = i // NZ, i % NZ
        q = zi // 2
        slot = q * 8 + 2 * turn_of(xi, q) + zi % 2
        high, low = split_bf16(vs[xi, zi] * columns[:, 8 * i : 8 * i + 1])
        grads[0, slot] = high
        grads[1, slot] = low

    half_to = y // 4

    def spans(i):
        if i == 2:
            return [(zh, 0), (zh, 1)]
        block = (half_to + 1 + i) % 2
        return [((zh + 1) % ZH, block), ((zh + 2) % ZH, block)]

    def row_grads(half, i):
        rows = [
            jnp.concatenate([et[k // 8][k % 8, half * (OWN // 256) + t * 2 + block] for k in range(CHIPS)], axis=1)
            for t, block in spans(i)
        ]
        right_side = jnp.concatenate([grads[k].reshape(CHIPS * B, D) for k in range(2)], axis=1)
        both = jnp.dot(jnp.concatenate(rows, axis=0), right_side, preferred_element_type=F32)
        return both[:, 0:D] + both[:, D:]

    l_out = [remote(lsend.at[i], lrecv.at[i], l_send.at[i], l_recv.at[i], partner) for i in range(3)]
    g_out = []
    for i in range(3):
        lsend[i] = row_grads(1 - c, i)
        l_out[i].start()
        total = row_grads(c, i)
        l_out[i].wait_recv()
        outb[i] = (total + lrecv[i]).reshape(NY, HOT, D)
        if i < 2:
            (t, block), (u, _) = spans(i)
            order = [
                (zz, part_of * 4 + (y + k) % 4, block * 4 + (y + k) % 4) for k in range(4) for part_of, zz in ((0, t), (1, u))
            ]
        else:
            order = [(zh, (y + o) % NY, (y + o) % NY) for o in range(1, NY)]
        for zz, k, yy in order:
            copy = remote(outb.at[i, k], grecv.at[g], g_send.at[len(g_out)], g_recv.at[g], (zz * NY + yy, s))
            copy.start()
            g_out.append(copy)
    grecv[g] = outb[2, y]
    for o in range(1, GROUPS):
        k = (g + o) % GROUPS
        remote(grecv.at[k], grecv.at[k], g_send.at[o - 1], g_recv.at[k], left).wait_recv()
    high, low = split_bf16(grecv[...].reshape(OWN, D))
    both = jnp.dot(
        jnp.concatenate([place_hot[i] for i in range(OWN // B)], axis=1),
        jnp.concatenate([high, low], axis=1),
        preferred_element_type=F32,
    )
    tgrad_ref[...] = (both[:, 0:D] + both[:, D:])[0:WIN]

    hot_out.wait_send()
    for copy in (*idx_out, *vz_out, *rs_out.values(), v_right, v_left, on_right, on_left):
        copy.wait_send()
    for copy in (*z_out, *pg_out, *l_out, *g_out):
        copy.wait_send()


def keep(*refs):
    for source, target in zip(refs[:3], refs[3:]):
        target[...] = source[...]


def on_device(bottom_out, lookups, starts, tables, top_dense, top_pairs, cotangent):
    vmem = pl.BlockSpec(memory_space=pltpu.VMEM)
    dma = pltpu.SemaphoreType.DMA
    hbm = pl.BlockSpec(memory_space=pltpu.HBM)
    shapes = (
        jax.ShapeDtypeStruct((B, 1024), BF16),
        jax.ShapeDtypeStruct((B, D), F32),
        jax.ShapeDtypeStruct((WIN, D), F32),
    )
    operands = (
        bottom_out, lookups[:, 0, :].T, top_pairs, starts, tables.reshape(GROUPS, WIN, D), top_dense, cotangent,
    )
    results = pl.pallas_call(
        kernel,
        out_shape=shapes,
        in_specs=[hbm] * 7,
        out_specs=(vmem, vmem, vmem),
        scratch_shapes=[
            pltpu.VMEM((B, D), BF16),
            pltpu.VMEM((4, B), I32),
            pltpu.VMEM((1, 1024), F32),
            pltpu.VMEM((D, 1024), BF16),
            pltpu.VMEM((B, 1024), F32),
            pltpu.SMEM((GROUPS, 256), I32),
            pltpu.VMEM((GROUPS, PAD, D), F32),
            pltpu.VMEM((ROWS, D), F32),
            pltpu.VMEM((ROWS // 128, 2 * D, 128), BF16),
            pltpu.VMEM((CHIPS, 8, B), I32),
            pltpu.VMEM((CHIPS // 2, ROWS // 256, 256, B), BF16),
            pltpu.VMEM((CHIPS // 2, ROWS // 256, 256, B), BF16),
            pltpu.VMEM((8, 2, D, B), F32),
            pltpu.VMEM((6, 2, D, B), F32),
            pltpu.VMEM((NZ, D, B), F32),
            pltpu.VMEM((NZ, D, B), F32),
            pltpu.VMEM((NX, NZ, B, D), F32),
            pltpu.VMEM((CHIPS, 8, B), F32),
            pltpu.VMEM((2, CHIPS, B, D), BF16),
            pltpu.VMEM((B, 1024), F32),
            pltpu.VMEM((ZH, NY * HOT, D), F32),
            pltpu.VMEM((ZH, NY * HOT, D), F32),
            pltpu.VMEM((ZH, NY, HOT, D), F32),
            pltpu.VMEM((GROUPS, HOT, D), F32),
            pltpu.VMEM((OWN // B, OUT_ROWS, B), BF16),
            dma((8,)), dma((2,)), dma((CHIPS - 1,)), dma((CHIPS,)), dma((NZ - 1,)), dma((NZ,)), dma((4,)), dma((4,)),
            dma((6,)), dma((6,)), dma((NZ - 1,)), dma((NZ,)), dma((CHIPS - 1,)), dma((CHIPS,)),
            dma((ZH,)), dma((ZH,)), dma((GROUPS - 1,)), dma((GROUPS,)),
        ],
        compiler_params=pltpu.CompilerParams(
            collective_id=0, has_side_effects=True, vmem_limit_bytes=38 * 1024 * 1024
        ),
    )(
        *(pltpu.with_memory_space_constraint(value, pltpu.HBM) for value in operands)
    )
    act, bgrad, tgrad = pl.pallas_call(
        keep,
        out_shape=shapes,
        in_specs=[vmem] * 3,
        out_specs=(vmem,) * 3,
        compiler_params=pltpu.CompilerParams(vmem_limit_bytes=4 * 1024 * 1024),
    )(*results)
    return act, bgrad, tgrad[None, None]


def solution(mesh):
    in_specs = (
        P(("grp", "shard"), None),
        P(("grp", "shard"), None, None),
        P(),
        P(None, "shard", None),
        P(),
        P(),
        P(("grp", "shard"), None),
    )
    out_specs = (
        P(("grp", "shard"), None),
        P(("grp", "shard"), None),
        P(None, "shard", "grp", None),
    )
    return jax.shard_map(
        on_device, mesh=mesh, in_specs=in_specs, out_specs=out_specs, check_vma=False
    )
```

```python
import jax
import jax.numpy as jnp
from jax import lax
from jax.experimental import pallas as pl
from jax.experimental.pallas import tpu as pltpu
from jax.sharding import PartitionSpec as P

HOT = 64
WIN = 328
NX, NZ, NC = 4, 4, 2
ZH, NY = 3, 8
CHIPS = NX * NZ
GROUPS = ZH * NY
B = 128
D = 128
OWN = GROUPS * HOT
ROWS = NC * OWN
PAD = WIN + HOT
OUT_ROWS = 336
F32, BF16, I32 = jnp.float32, jnp.bfloat16, jnp.int32
MESH = pl.DeviceIdType.MESH


def split_bf16(value):
    high = value.astype(BF16)
    return high, (value - high.astype(F32)).astype(BF16)


def kernel(
    bottom_hbm, lookups_hbm, pairs_hbm, starts_ref, tables_ref, dense_hbm, cot_hbm,
    act_ref, bgrad_ref, tgrad_ref,
    bottom_ref, lookups_ref, pairs_ref, dense_ref, cot_ref, start_of, win, hot, hot_t, idxs, et_a, et_b, part, rx, qz, zr, vs, pgs, grads, pre_dense, lsend, lrecv, outb, grecv, place_hot,
    local_sem, hot_sem, idx_send, idx_recv, vz_send, vz_recv, far_send, far_recv, vx_send, vx_recv,
    rs_send, rs_recv, z_send, z_recv, pg_send, pg_recv, l_send, l_recv, g_send, g_recv,
):
    g = lax.axis_index("grp")
    s = lax.axis_index("shard")
    zh, y = g // NY, g % NY
    et = (et_a, et_b)
    c = s % NC
    chip = s // NC
    x, z = chip // NZ, chip % NZ

    def at(chip_to):
        return (g, chip_to * NC + c)

    right = at((x + 1) % NX * NZ + z)
    left = at((x + NX - 1) % NX * NZ + z)
    partner = (g, chip * NC + (1 - c))

    def remote(src, dst, send, recv, to):
        return pltpu.make_async_remote_copy(
            src_ref=src, dst_ref=dst, send_sem=send, recv_sem=recv, device_id=to, device_id_type=MESH
        )

    first = (s * GROUPS // 128 - s // 27) * 128
    starts_in = pltpu.make_async_copy(starts_ref.at[:, pl.ds(pl.multiple_of(first, 128), 256)], start_of, local_sem.at[2])
    whole = pltpu.make_async_copy(tables_ref, win.at[:, pl.ds(0, WIN)], local_sem.at[0])
    again = pltpu.make_async_copy(tables_ref.at[:, pl.ds(0, HOT)], win.at[:, pl.ds(WIN, HOT)], local_sem.at[1])
    dense_in = pltpu.make_async_copy(dense_hbm, dense_ref, local_sem.at[3])
    cot_in = pltpu.make_async_copy(cot_hbm, cot_ref, local_sem.at[4])
    lookups_in = pltpu.make_async_copy(lookups_hbm, lookups_ref, local_sem.at[5])
    bottom_in = pltpu.make_async_copy(bottom_hbm, bottom_ref, local_sem.at[6])
    pairs_in = pltpu.make_async_copy(pairs_hbm, pairs_ref, local_sem.at[7])
    for copy in (lookups_in, bottom_in, starts_in, whole, again, dense_in, cot_in, pairs_in):
        copy.start()

    barrier = pltpu.get_barrier_semaphore()
    pl.semaphore_signal(barrier, inc=1, device_id=partner, device_id_type=MESH)
    for o in range(1, CHIPS):
        pl.semaphore_signal(barrier, inc=1, device_id=at((chip + o) % CHIPS), device_id_type=MESH)
    for o in range(1, GROUPS):
        pl.semaphore_signal(barrier, inc=1, device_id=((g + o) % GROUPS, s), device_id_type=MESH)

    lookups_in.wait()
    picked = lookups_ref[...]
    window = ((picked.astype(F32) + 0.5) * (1.0 / WIN)).astype(I32)
    hot_index = picked - window * (WIN - HOT)
    counts = jnp.zeros((4, B), I32)
    for k in range(4):
        counts = counts + jnp.where(hot_index == hot_index[k : k + 1], 1, 0)
    idxs[chip, 0:4] = hot_index
    idxs[chip, 4:8] = counts
    bottom_in.wait()
    vs[x, z] = bottom_ref[...].astype(F32)
    pl.semaphore_wait(barrier, 1 + CHIPS - 1 + GROUPS - 1)

    idx_out = [
        remote(idxs.at[chip], idxs.at[chip], idx_send.at[o - 1], idx_recv.at[chip], at((chip + o) % CHIPS))
        for o in range(1, CHIPS)
    ]
    for copy in idx_out:
        copy.start()
    vz_out = [
        remote(vs.at[x, z], vs.at[x, z], vz_send.at[o - 1], vz_recv.at[z], at(x * NZ + (z + o) % NZ))
        for o in range(1, NZ)
    ]
    for copy in vz_out:
        copy.start()
    x_far = (x + 2) % NX
    far_out = remote(vs.at[x, z], vs.at[x, z], far_send.at[NZ - 1], far_recv.at[z], at(x_far * NZ + z))
    far_out.start()
    far_on = [
        remote(vs.at[x_far, z], vs.at[x_far, z], far_send.at[o - 1], far_recv.at[z], at(x * NZ + (z + o) % NZ))
        for o in range(1, NZ)
    ]
    starts_in.wait()
    whole.wait()
    again.wait()
    for w in range(GROUPS):
        hot[pl.ds(c * OWN + w * HOT, HOT)] = win[w, pl.ds(start_of[g, s * GROUPS - first + w], HOT), :]
    mine = hot.at[pl.ds(c * OWN, OWN)]
    hot_out = remote(mine, mine, hot_sem.at[0], hot_sem.at[1], partner)
    hot_out.start()

    def turn_hot(half):
        def step(i, carry):
            at_row = pl.multiple_of(half * OWN + i * 128, 128)
            tile = hot[pl.ds(at_row, 128), :].T
            high, low = split_bf16(tile)
            hot_t[half * GROUPS // 2 + i, 0:D] = high
            hot_t[half * GROUPS // 2 + i, D:] = low
            return carry

        lax.fori_loop(0, OWN // 128, step, 0, unroll=4)

    turn_hot(c)
    dense_in.wait()
    pre_dense[...] = jnp.dot(bottom_ref[...], dense_ref[...], preferred_element_type=F32)
    hot_out.wait_recv()
    turn_hot(1 - c)

    def await_idx(k):
        remote(idxs.at[k], idxs.at[k], idx_send.at[0], idx_recv.at[k], left).wait_recv()

    for o in range(1, NZ):
        await_idx(x * NZ + (z + o) % NZ)

    row_iota = lax.broadcasted_iota(I32, (256, B), 0).astype(F32).astype(BF16)

    rs_to = {0: right, 1: left, 2: left, 3: right, 4: right, 5: left}
    rs_out = {p: remote(part.at[p], rx.at[p], rs_send.at[p], rs_recv.at[p], to) for p, to in rs_to.items()}

    def x_of(h, q):
        return (x + (2 + h + h // 2 * (2 * h - 3)) * (1 + 2 * q)) % NX

    def turn_of(xx, q):
        m = ((xx - x + NX) * (1 + 2 * q) + 2) % NX
        return m + m // 2 * (5 - 2 * m)

    def build(h, q):
        xx = x_of(h, q)
        for b in range(2):
            rows = idxs[xx * NZ + 2 * q + b]
            local = rows[0:4] - chip * ROWS
            counts = rows[4:8].astype(F32).astype(BF16)
            for j in range(ROWS // 256):
                near = jnp.clip(local - j * 256, -1, 256).astype(F32).astype(BF16)
                tile = jnp.zeros((256, B), BF16)
                for k in range(4):
                    tile = jnp.where(row_iota == near[k : k + 1], counts[k : k + 1], tile)
                et[q][2 * h + b, j] = tile

    def pool(h, q):
        both = jnp.dot(
            jnp.concatenate([hot_t[i] for i in range(ROWS // 128)], axis=1),
            jnp.concatenate([et[q][2 * h + b].reshape(ROWS, B) for b in range(2)], axis=1),
            preferred_element_type=F32,
        )
        summed = both[0:D] + both[D:]
        part[2 * h + q, 0] = summed[:, 0:B]
        part[2 * h + q, 1] = summed[:, B:]

    def pass_on(h, q):
        for k in rs_out:
            if k % 2 == q:

                @pl.when(h == k // 2)
                def _():
                    if k >= 4:
                        rs_out[k - 4].wait_recv()
                        part[k] = part[k] + rx[k - 4]
                    rs_out[k].start()
                    if k == 0:
                        remote(vs.at[x_far, z], vs.at[x_far, z], far_send.at[0], far_recv.at[z], left).wait_recv()
                        for copy in far_on:
                            copy.start()
                    if k == 5:
                        for o in range(1, NZ):
                            kz = (z + o) % NZ
                            remote(vs.at[x, kz], vs.at[x, kz], vz_send.at[o - 1], vz_recv.at[kz], left).wait_recv()
                        v_right.start()
                        v_left.start()

    v_right = remote(vs.at[x], vs.at[x], vx_send.at[0], vx_recv.at[0], right)
    v_left = remote(vs.at[x], vs.at[x], vx_send.at[1], vx_recv.at[1], left)

    for b in range(2):
        await_idx(x_far * NZ + b)
    build(0, 0)

    def pool_step(h, carry):
        @pl.when(h < 3)
        def _():
            for b in range(2):
                await_idx(x_of(h, 1) * NZ + 2 + b)

        build(h, 1)
        pool(h, 0)
        pass_on(h, 0)

        @pl.when(h < 2)
        def _():
            for b in range(2):
                await_idx(x_of(h + 1, 0) * NZ + b)

        build((h + 1) % 4, 0)
        pool(h, 1)
        pass_on(h, 1)
        return carry

    lax.fori_loop(0, 4, pool_step, 0)

    for q in range(2):
        a, b = (2, 4) if q == 0 else (3, 5)
        rs_out[a].wait_recv()
        rs_out[b].wait_recv()
        qz[pl.ds(2 * q, 2)] = part[6 + q] + rx[a] + rx[b]
    z_out = [
        remote(qz.at[(z + o) % NZ], zr.at[z], z_send.at[o - 1], z_recv.at[z], at(x * NZ + (z + o) % NZ))
        for o in range(1, NZ)
    ]
    for copy in z_out:
        copy.start()

    place_iota = lax.broadcasted_iota(I32, (OUT_ROWS, B), 0)
    lane = lax.broadcasted_iota(I32, (1, B), 1)
    column = s * GROUPS - first + g
    for i in range(OWN // B):
        place = lane % HOT + jnp.where(lane < HOT, start_of[2 * i, column], start_of[2 * i + 1, column])
        place = jnp.where(place >= WIN, place - WIN, place)
        place_hot[i] = jnp.where(place_iota == place, 1.0, 0.0).astype(BF16)

    pooled_t = qz[z]
    for o in range(1, NZ):
        k = (z + o) % NZ
        remote(qz.at[k], zr.at[k], z_send.at[o - 1], z_recv.at[k], left).wait_recv()
        pooled_t = pooled_t + zr[k]
    pooled = pooled_t.T

    v0 = bottom_ref[...].astype(F32)
    cot_in.wait()
    pairs_in.wait()
    pair_dots = jnp.sum(v0 * pooled, axis=1, keepdims=True)
    preact = pre_dense[...] + pair_dots * pairs_ref[...]
    gate = jax.nn.sigmoid(preact)
    pre_grad = cot_ref[...] * gate * (1.0 + preact * (1.0 - gate))
    pair_grad = jnp.sum(pre_grad * pairs_ref[...], axis=1, keepdims=True)
    pgs[chip] = jnp.broadcast_to(pair_grad, (B, B)).T[0:8]
    pg_out = [
        remote(pgs.at[chip], pgs.at[chip], pg_send.at[o - 1], pg_recv.at[chip], at((chip + o) % CHIPS))
        for o in range(1, CHIPS)
    ]
    for copy in pg_out:
        copy.start()
    act_ref[...] = (preact * gate).astype(BF16)
    bgrad_ref[...] = (
        lax.dot_general(
            pre_grad.astype(BF16), dense_ref[...], (((1,), (1,)), ((), ())), preferred_element_type=F32
        )
        + pair_grad * pooled
    )

    v_right.wait_recv()
    v_left.wait_recv()
    for o in range(1, NZ):
        k = (z + o) % NZ
        remote(vs.at[x_far, k], vs.at[x_far, k], far_send.at[0], far_recv.at[k], left).wait_recv()
    for o in range(1, CHIPS):
        k = (chip + o) % CHIPS
        remote(pgs.at[k], pgs.at[k], pg_send.at[o - 1], pg_recv.at[k], left).wait_recv()
    columns = pgs[...].reshape(CHIPS * 8, B).T
    for i in range(CHIPS):
        xi, zi = i // NZ, i % NZ
        q = zi // 2
        slot = q * 8 + 2 * turn_of(xi, q) + zi % 2
        high, low = split_bf16(vs[xi, zi] * columns[:, 8 * i : 8 * i + 1])
        grads[0, slot] = high
        grads[1, slot] = low

    parts = [(zh + 1 + z // 2) % ZH, (zh + 2 + 2 * (z // 2)) % ZH, zh]

    def row_grads(half, i):
        rows = [
            jnp.concatenate([et[k // 8][k % 8, half * (OWN // 256) + t * 2 + block] for k in range(CHIPS)], axis=1)
            for t, block in ((parts[i], 0), (parts[i], 1))
        ]
        right_side = jnp.concatenate([grads[k].reshape(CHIPS * B, D) for k in range(2)], axis=1)
        both = jnp.dot(jnp.concatenate(rows, axis=0), right_side, preferred_element_type=F32)
        return both[:, 0:D] + both[:, D:]

    l_out = [remote(lsend.at[i], lrecv.at[i], l_send.at[i], l_recv.at[i], partner) for i in range(3)]
    g_out = []
    for i in range(3):
        lsend[i] = row_grads(1 - c, i)
        l_out[i].start()
        total = row_grads(c, i)
        l_out[i].wait_recv()
        outb[i] = (total + lrecv[i]).reshape(NY, HOT, D)
        for o in (1, 7, 2, 6, 3, 5, 4, 0):
            if i == 2 and o == 0:
                continue
            k = (y + o) % NY
            copy = remote(outb.at[i, k], grecv.at[g], g_send.at[len(g_out)], g_recv.at[g], (parts[i] * NY + k, s))
            copy.start()
            g_out.append(copy)
    grecv[g] = outb[2, y]
    for o in range(1, GROUPS):
        k = (g + o) % GROUPS
        remote(grecv.at[k], grecv.at[k], g_send.at[o - 1], g_recv.at[k], left).wait_recv()
    high, low = split_bf16(grecv[...].reshape(OWN, D))
    both = jnp.dot(
        jnp.concatenate([place_hot[i] for i in range(OWN // B)], axis=1),
        jnp.concatenate([high, low], axis=1),
        preferred_element_type=F32,
    )
    tgrad_ref[...] = (both[:, 0:D] + both[:, D:])[0:WIN]

    hot_out.wait_send()
    for copy in (*idx_out, *vz_out, *rs_out.values(), v_right, v_left, far_out, *far_on):
        copy.wait_send()
    for copy in (*z_out, *pg_out, *l_out, *g_out):
        copy.wait_send()


def keep(*refs):
    for source, target in zip(refs[:3], refs[3:]):
        target[...] = source[...]


def on_device(bottom_out, lookups, starts, tables, top_dense, top_pairs, cotangent):
    vmem = pl.BlockSpec(memory_space=pltpu.VMEM)
    dma = pltpu.SemaphoreType.DMA
    hbm = pl.BlockSpec(memory_space=pltpu.HBM)
    shapes = (
        jax.ShapeDtypeStruct((B, 1024), BF16),
        jax.ShapeDtypeStruct((B, D), F32),
        jax.ShapeDtypeStruct((WIN, D), F32),
    )
    operands = (
        bottom_out, lookups[:, 0, :].T, top_pairs, starts, tables.reshape(GROUPS, WIN, D), top_dense, cotangent,
    )
    results = pl.pallas_call(
        kernel,
        out_shape=shapes,
        in_specs=[hbm] * 7,
        out_specs=(vmem, vmem, vmem),
        scratch_shapes=[
            pltpu.VMEM((B, D), BF16),
            pltpu.VMEM((4, B), I32),
            pltpu.VMEM((1, 1024), F32),
            pltpu.VMEM((D, 1024), BF16),
            pltpu.VMEM((B, 1024), F32),
            pltpu.SMEM((GROUPS, 256), I32),
            pltpu.VMEM((GROUPS, PAD, D), F32),
            pltpu.VMEM((ROWS, D), F32),
            pltpu.VMEM((ROWS // 128, 2 * D, 128), BF16),
            pltpu.VMEM((CHIPS, 8, B), I32),
            pltpu.VMEM((CHIPS // 2, ROWS // 256, 256, B), BF16),
            pltpu.VMEM((CHIPS // 2, ROWS // 256, 256, B), BF16),
            pltpu.VMEM((8, 2, D, B), F32),
            pltpu.VMEM((6, 2, D, B), F32),
            pltpu.VMEM((NZ, D, B), F32),
            pltpu.VMEM((NZ, D, B), F32),
            pltpu.VMEM((NX, NZ, B, D), F32),
            pltpu.VMEM((CHIPS, 8, B), F32),
            pltpu.VMEM((2, CHIPS, B, D), BF16),
            pltpu.VMEM((B, 1024), F32),
            pltpu.VMEM((ZH, NY * HOT, D), F32),
            pltpu.VMEM((ZH, NY * HOT, D), F32),
            pltpu.VMEM((ZH, NY, HOT, D), F32),
            pltpu.VMEM((GROUPS, HOT, D), F32),
            pltpu.VMEM((OWN // B, OUT_ROWS, B), BF16),
            dma((8,)), dma((2,)), dma((CHIPS - 1,)), dma((CHIPS,)), dma((NZ - 1,)), dma((NZ,)), dma((NZ,)), dma((NZ,)), dma((2,)), dma((2,)),
            dma((6,)), dma((6,)), dma((NZ - 1,)), dma((NZ,)), dma((CHIPS - 1,)), dma((CHIPS,)),
            dma((ZH,)), dma((ZH,)), dma((GROUPS - 1,)), dma((GROUPS,)),
        ],
        compiler_params=pltpu.CompilerParams(
            collective_id=0, has_side_effects=True, vmem_limit_bytes=38 * 1024 * 1024
        ),
    )(
        *(pltpu.with_memory_space_constraint(value, pltpu.HBM) for value in operands)
    )
    act, bgrad, tgrad = pl.pallas_call(
        keep,
        out_shape=shapes,
        in_specs=[vmem] * 3,
        out_specs=(vmem,) * 3,
        compiler_params=pltpu.CompilerParams(vmem_limit_bytes=4 * 1024 * 1024),
    )(*results)
    return act, bgrad, tgrad[None, None]


def solution(mesh):
    in_specs = (
        P(("grp", "shard"), None),
        P(("grp", "shard"), None, None),
        P(),
        P(None, "shard", None),
        P(),
        P(),
        P(("grp", "shard"), None),
    )
    out_specs = (
        P(("grp", "shard"), None),
        P(("grp", "shard"), None),
        P(None, "shard", "grp", None),
    )
    return jax.shard_map(
        on_device, mesh=mesh, in_specs=in_specs, out_specs=out_specs, check_vma=False
    )
```

```python
import jax
import jax.numpy as jnp
from jax import lax
from jax.experimental import pallas as pl
from jax.experimental.pallas import tpu as pltpu
from jax.sharding import PartitionSpec as P

HOT = 64
WIN = 328
NX, NZ, NC = 4, 4, 2
ZH, NY = 3, 8
CHIPS = NX * NZ
GROUPS = ZH * NY
B = 128
D = 128
OWN = GROUPS * HOT
ROWS = NC * OWN
PAD = WIN + HOT
OUT_ROWS = 336
F32, BF16, I32 = jnp.float32, jnp.bfloat16, jnp.int32
MESH = pl.DeviceIdType.MESH


def split_bf16(value):
    high = value.astype(BF16)
    return high, (value - high.astype(F32)).astype(BF16)


def kernel(
    bottom_hbm, lookups_hbm, pairs_hbm, starts_ref, tables_ref, dense_hbm, cot_hbm,
    act_ref, bgrad_ref, tgrad_ref,
    bottom_ref, lookups_ref, pairs_ref, dense_ref, cot_ref, start_of, win, hot, hot_t, idxs, et_a, et_b, part, rx, qz, zr, vs, pgs, grads, pre_dense, lsend, lrecv, outb, grecv, place_hot,
    local_sem, hot_sem, idx_send, idx_recv, vz_send, vz_recv, far_send, far_recv, vx_send, vx_recv,
    rs_send, rs_recv, z_send, z_recv, pg_send, pg_recv, l_send, l_recv, g_send, g_recv,
):
    g = lax.axis_index("grp")
    s = lax.axis_index("shard")
    zh, y = g // NY, g % NY
    et = (et_a, et_b)
    c = s % NC
    chip = s // NC
    x, z = chip // NZ, chip % NZ

    def at(chip_to):
        return (g, chip_to * NC + c)

    right = at((x + 1) % NX * NZ + z)
    left = at((x + NX - 1) % NX * NZ + z)
    partner = (g, chip * NC + (1 - c))

    def remote(src, dst, send, recv, to):
        return pltpu.make_async_remote_copy(
            src_ref=src, dst_ref=dst, send_sem=send, recv_sem=recv, device_id=to, device_id_type=MESH
        )

    first = (s * GROUPS // 128 - s // 27) * 128
    starts_in = pltpu.make_async_copy(starts_ref.at[:, pl.ds(pl.multiple_of(first, 128), 256)], start_of, local_sem.at[2])
    whole = pltpu.make_async_copy(tables_ref, win.at[:, pl.ds(0, WIN)], local_sem.at[0])
    again = pltpu.make_async_copy(tables_ref.at[:, pl.ds(0, HOT)], win.at[:, pl.ds(WIN, HOT)], local_sem.at[1])
    dense_in = pltpu.make_async_copy(dense_hbm, dense_ref, local_sem.at[3])
    cot_in = pltpu.make_async_copy(cot_hbm, cot_ref, local_sem.at[4])
    lookups_in = pltpu.make_async_copy(lookups_hbm, lookups_ref, local_sem.at[5])
    bottom_in = pltpu.make_async_copy(bottom_hbm, bottom_ref, local_sem.at[6])
    pairs_in = pltpu.make_async_copy(pairs_hbm, pairs_ref, local_sem.at[7])
    for copy in (lookups_in, bottom_in, starts_in, whole, again, dense_in, cot_in, pairs_in):
        copy.start()

    barrier = pltpu.get_barrier_semaphore()
    pl.semaphore_signal(barrier, inc=1, device_id=partner, device_id_type=MESH)
    for o in range(1, CHIPS):
        pl.semaphore_signal(barrier, inc=1, device_id=at((chip + o) % CHIPS), device_id_type=MESH)
    for o in range(1, GROUPS):
        pl.semaphore_signal(barrier, inc=1, device_id=((g + o) % GROUPS, s), device_id_type=MESH)

    lookups_in.wait()
    picked = lookups_ref[...]
    window = ((picked.astype(F32) + 0.5) * (1.0 / WIN)).astype(I32)
    hot_index = picked - window * (WIN - HOT)
    counts = jnp.zeros((4, B), I32)
    for k in range(4):
        counts = counts + jnp.where(hot_index == hot_index[k : k + 1], 1, 0)
    idxs[chip, 0:4] = hot_index
    idxs[chip, 4:8] = counts
    bottom_in.wait()
    vs[x, z] = bottom_ref[...].astype(F32)
    pl.semaphore_wait(barrier, 1 + CHIPS - 1 + GROUPS - 1)

    idx_out = [
        remote(idxs.at[chip], idxs.at[chip], idx_send.at[o - 1], idx_recv.at[chip], at((chip + o) % CHIPS))
        for o in range(1, CHIPS)
    ]
    for copy in idx_out:
        copy.start()
    vz_out = [
        remote(vs.at[x, z], vs.at[x, z], vz_send.at[o - 1], vz_recv.at[z], at(x * NZ + (z + o) % NZ))
        for o in range(1, NZ)
    ]
    for copy in vz_out:
        copy.start()
    x_far = (x + 2) % NX
    far_out = remote(vs.at[x, z], vs.at[x, z], far_send.at[NZ - 1], far_recv.at[z], at(x_far * NZ + z))
    far_out.start()
    far_on = [
        remote(vs.at[x_far, z], vs.at[x_far, z], far_send.at[o - 1], far_recv.at[z], at(x * NZ + (z + o) % NZ))
        for o in range(1, NZ)
    ]
    starts_in.wait()
    whole.wait()
    again.wait()
    for w in range(GROUPS):
        hot[pl.ds(c * OWN + w * HOT, HOT)] = win[w, pl.ds(start_of[g, s * GROUPS - first + w], HOT), :]
    mine = hot.at[pl.ds(c * OWN, OWN)]
    hot_out = remote(mine, mine, hot_sem.at[0], hot_sem.at[1], partner)
    hot_out.start()

    def turn_hot(half):
        def step(i, carry):
            at_row = pl.multiple_of(half * OWN + i * 128, 128)
            tile = hot[pl.ds(at_row, 128), :].T
            high, low = split_bf16(tile)
            hot_t[half * GROUPS // 2 + i, 0:D] = high
            hot_t[half * GROUPS // 2 + i, D:] = low
            return carry

        lax.fori_loop(0, OWN // 128, step, 0, unroll=4)

    turn_hot(c)
    dense_in.wait()
    pre_dense[...] = jnp.dot(bottom_ref[...], dense_ref[...], preferred_element_type=F32)
    hot_out.wait_recv()
    turn_hot(1 - c)

    def await_idx(k):
        remote(idxs.at[k], idxs.at[k], idx_send.at[0], idx_recv.at[k], left).wait_recv()

    for o in range(1, NZ):
        await_idx(x * NZ + (z + o) % NZ)

    row_iota = lax.broadcasted_iota(I32, (256, B), 0).astype(F32).astype(BF16)

    rs_to = {0: right, 1: left, 2: left, 3: right, 4: right, 5: left}
    rs_out = {p: remote(part.at[p], rx.at[p], rs_send.at[p], rs_recv.at[p], to) for p, to in rs_to.items()}

    def x_of(h, q):
        return (x + (2 + h + h // 2 * (2 * h - 3)) * (1 + 2 * q)) % NX

    def turn_of(xx, q):
        m = ((xx - x + NX) * (1 + 2 * q) + 2) % NX
        return m + m // 2 * (5 - 2 * m)

    def build(h, q):
        xx = x_of(h, q)
        for b in range(2):
            rows = idxs[xx * NZ + 2 * q + b]
            local = rows[0:4] - chip * ROWS
            counts = rows[4:8].astype(F32).astype(BF16)
            for j in range(ROWS // 256):
                near = jnp.clip(local - j * 256, -1, 256).astype(F32).astype(BF16)
                tile = jnp.zeros((256, B), BF16)
                for k in range(4):
                    tile = jnp.where(row_iota == near[k : k + 1], counts[k : k + 1], tile)
                et[q][2 * h + b, j] = tile

    def pool(h, q):
        both = jnp.dot(
            jnp.concatenate([hot_t[i] for i in range(ROWS // 128)], axis=1),
            jnp.concatenate([et[q][2 * h + b].reshape(ROWS, B) for b in range(2)], axis=1),
            preferred_element_type=F32,
        )
        summed = both[0:D] + both[D:]
        part[2 * h + q, 0] = summed[:, 0:B]
        part[2 * h + q, 1] = summed[:, B:]

    def pass_on(h, q):
        for k in rs_out:
            if k % 2 == q:

                @pl.when(h == k // 2)
                def _():
                    if k >= 4:
                        rs_out[k - 4].wait_recv()
                        part[k] = part[k] + rx[k - 4]
                    rs_out[k].start()
                    if k == 0:
                        remote(vs.at[x_far, z], vs.at[x_far, z], far_send.at[0], far_recv.at[z], left).wait_recv()
                        for copy in far_on:
                            copy.start()

    v_right = remote(vs.at[x], vs.at[x], vx_send.at[0], vx_recv.at[0], right)
    v_left = remote(vs.at[x], vs.at[x], vx_send.at[1], vx_recv.at[1], left)

    for b in range(2):
        await_idx(x_far * NZ + b)
    build(0, 0)

    def pool_step(h, carry):
        @pl.when(h < 3)
        def _():
            for b in range(2):
                await_idx(x_of(h, 1) * NZ + 2 + b)

        build(h, 1)
        pool(h, 0)
        pass_on(h, 0)

        @pl.when(h < 2)
        def _():
            for b in range(2):
                await_idx(x_of(h + 1, 0) * NZ + b)

        build((h + 1) % 4, 0)
        pool(h, 1)
        pass_on(h, 1)
        return carry

    lax.fori_loop(0, 4, pool_step, 0)

    for q in range(2):
        a, b = (2, 4) if q == 0 else (3, 5)
        rs_out[a].wait_recv()
        rs_out[b].wait_recv()
        qz[pl.ds(2 * q, 2)] = part[6 + q] + rx[a] + rx[b]
        for k in (2 * q, 2 * q + 1):

            @pl.when(z != k)
            def _():
                remote(qz.at[k], zr.at[z], z_send.at[k], z_recv.at[z], at(x * NZ + k)).start()

    for o in range(1, NZ):
        k = (z + o) % NZ
        remote(vs.at[x, k], vs.at[x, k], vz_send.at[o - 1], vz_recv.at[k], left).wait_recv()
    v_right.start()
    v_left.start()

    place_iota = lax.broadcasted_iota(I32, (OUT_ROWS, B), 0)
    lane = lax.broadcasted_iota(I32, (1, B), 1)
    column = s * GROUPS - first + g
    for i in range(OWN // B):
        place = lane % HOT + jnp.where(lane < HOT, start_of[2 * i, column], start_of[2 * i + 1, column])
        place = jnp.where(place >= WIN, place - WIN, place)
        place_hot[i] = jnp.where(place_iota == place, 1.0, 0.0).astype(BF16)

    pooled_t = qz[z]
    for o in range(1, NZ):
        k = (z + o) % NZ
        remote(qz.at[k], zr.at[k], z_send.at[0], z_recv.at[k], left).wait_recv()
        pooled_t = pooled_t + zr[k]
    pooled = pooled_t.T

    v0 = bottom_ref[...].astype(F32)
    cot_in.wait()
    pairs_in.wait()
    pair_dots = jnp.sum(v0 * pooled, axis=1, keepdims=True)
    preact = pre_dense[...] + pair_dots * pairs_ref[...]
    gate = jax.nn.sigmoid(preact)
    pre_grad = cot_ref[...] * gate * (1.0 + preact * (1.0 - gate))
    pair_grad = jnp.sum(pre_grad * pairs_ref[...], axis=1, keepdims=True)
    pgs[chip] = jnp.broadcast_to(pair_grad, (B, B)).T[0:8]
    pg_out = [
        remote(pgs.at[chip], pgs.at[chip], pg_send.at[o - 1], pg_recv.at[chip], at((chip + o) % CHIPS))
        for o in range(1, CHIPS)
    ]
    for copy in pg_out:
        copy.start()
    act_ref[...] = (preact * gate).astype(BF16)
    bgrad_ref[...] = (
        lax.dot_general(
            pre_grad.astype(BF16), dense_ref[...], (((1,), (1,)), ((), ())), preferred_element_type=F32
        )
        + pair_grad * pooled
    )

    v_right.wait_recv()
    v_left.wait_recv()
    for o in range(1, NZ):
        k = (z + o) % NZ
        remote(vs.at[x_far, k], vs.at[x_far, k], far_send.at[0], far_recv.at[k], left).wait_recv()
    for o in range(1, CHIPS):
        k = (chip + o) % CHIPS
        remote(pgs.at[k], pgs.at[k], pg_send.at[o - 1], pg_recv.at[k], left).wait_recv()
    columns = pgs[...].reshape(CHIPS * 8, B).T
    for i in range(CHIPS):
        xi, zi = i // NZ, i % NZ
        q = zi // 2
        slot = q * 8 + 2 * turn_of(xi, q) + zi % 2
        high, low = split_bf16(vs[xi, zi] * columns[:, 8 * i : 8 * i + 1])
        grads[0, slot] = high
        grads[1, slot] = low

    def row_grads(half, i):
        rows = [
            jnp.concatenate([et[k // 8][k % 8, half * (OWN // 256) + i * 2 + block] for k in range(CHIPS)], axis=1)
            for block in range(2)
        ]
        right_side = jnp.concatenate([grads[k].reshape(CHIPS * B, D) for k in range(2)], axis=1)
        both = jnp.dot(jnp.concatenate(rows, axis=0), right_side, preferred_element_type=F32)
        return both[:, 0:D] + both[:, D:]

    l_out = [remote(lsend.at[i], lrecv.at[i], l_send.at[i], l_recv.at[i], partner) for i in range(3)]
    g_out = []
    for i in range(3):
        lsend[i] = row_grads(1 - c, i)
        l_out[i].start()
        total = row_grads(c, i)
        l_out[i].wait_recv()
        outb[i] = (total + lrecv[i]).reshape(NY, HOT, D)
        for o in (1, 7, 2, 6, 3, 5, 4):
            k = (y + o) % NY
            copy = remote(outb.at[i, k], grecv.at[g], g_send.at[i * NY + o], g_recv.at[g], (i * NY + k, s))
            copy.start()
            g_out.append(copy)

        @pl.when(i != zh)
        def _():
            remote(outb.at[i, y], grecv.at[g], g_send.at[i * NY], g_recv.at[g], (i * NY + y, s)).start()

    grecv[g] = outb[zh, y]
    for o in range(1, GROUPS):
        k = (g + o) % GROUPS
        remote(grecv.at[k], grecv.at[k], g_send.at[0], g_recv.at[k], left).wait_recv()
    high, low = split_bf16(grecv[...].reshape(OWN, D))
    both = jnp.dot(
        jnp.concatenate([place_hot[i] for i in range(OWN // B)], axis=1),
        jnp.concatenate([high, low], axis=1),
        preferred_element_type=F32,
    )
    tgrad_ref[...] = (both[:, 0:D] + both[:, D:])[0:WIN]

    hot_out.wait_send()
    for copy in (*idx_out, *vz_out, *rs_out.values(), v_right, v_left, far_out, *far_on):
        copy.wait_send()
    for copy in (*pg_out, *l_out, *g_out):
        copy.wait_send()
    for o in range(1, NZ):
        k = (z + o) % NZ
        remote(qz.at[k], zr.at[z], z_send.at[k], z_recv.at[z], at(x * NZ + k)).wait_send()
    for o in range(1, ZH):
        t = (zh + o) % ZH
        remote(outb.at[t, y], grecv.at[g], g_send.at[t * NY], g_recv.at[g], (t * NY + y, s)).wait_send()


def keep(*refs):
    for source, target in zip(refs[:3], refs[3:]):
        target[...] = source[...]


def on_device(bottom_out, lookups, starts, tables, top_dense, top_pairs, cotangent):
    vmem = pl.BlockSpec(memory_space=pltpu.VMEM)
    dma = pltpu.SemaphoreType.DMA
    hbm = pl.BlockSpec(memory_space=pltpu.HBM)
    shapes = (
        jax.ShapeDtypeStruct((B, 1024), BF16),
        jax.ShapeDtypeStruct((B, D), F32),
        jax.ShapeDtypeStruct((WIN, D), F32),
    )
    operands = (
        bottom_out, lookups[:, 0, :].T, top_pairs, starts, tables.reshape(GROUPS, WIN, D), top_dense, cotangent,
    )
    results = pl.pallas_call(
        kernel,
        out_shape=shapes,
        in_specs=[hbm] * 7,
        out_specs=(vmem, vmem, vmem),
        scratch_shapes=[
            pltpu.VMEM((B, D), BF16),
            pltpu.VMEM((4, B), I32),
            pltpu.VMEM((1, 1024), F32),
            pltpu.VMEM((D, 1024), BF16),
            pltpu.VMEM((B, 1024), F32),
            pltpu.SMEM((GROUPS, 256), I32),
            pltpu.VMEM((GROUPS, PAD, D), F32),
            pltpu.VMEM((ROWS, D), F32),
            pltpu.VMEM((ROWS // 128, 2 * D, 128), BF16),
            pltpu.VMEM((CHIPS, 8, B), I32),
            pltpu.VMEM((CHIPS // 2, ROWS // 256, 256, B), BF16),
            pltpu.VMEM((CHIPS // 2, ROWS // 256, 256, B), BF16),
            pltpu.VMEM((8, 2, D, B), F32),
            pltpu.VMEM((6, 2, D, B), F32),
            pltpu.VMEM((NZ, D, B), F32),
            pltpu.VMEM((NZ, D, B), F32),
            pltpu.VMEM((NX, NZ, B, D), F32),
            pltpu.VMEM((CHIPS, 8, B), F32),
            pltpu.VMEM((2, CHIPS, B, D), BF16),
            pltpu.VMEM((B, 1024), F32),
            pltpu.VMEM((ZH, NY * HOT, D), F32),
            pltpu.VMEM((ZH, NY * HOT, D), F32),
            pltpu.VMEM((ZH, NY, HOT, D), F32),
            pltpu.VMEM((GROUPS, HOT, D), F32),
            pltpu.VMEM((OWN // B, OUT_ROWS, B), BF16),
            dma((8,)), dma((2,)), dma((CHIPS - 1,)), dma((CHIPS,)), dma((NZ - 1,)), dma((NZ,)), dma((NZ,)), dma((NZ,)), dma((2,)), dma((2,)),
            dma((6,)), dma((6,)), dma((NZ,)), dma((NZ,)), dma((CHIPS - 1,)), dma((CHIPS,)),
            dma((ZH,)), dma((ZH,)), dma((GROUPS,)), dma((GROUPS,)),
        ],
        compiler_params=pltpu.CompilerParams(
            collective_id=0, has_side_effects=True, vmem_limit_bytes=38 * 1024 * 1024
        ),
    )(
        *(pltpu.with_memory_space_constraint(value, pltpu.HBM) for value in operands)
    )
    act, bgrad, tgrad = pl.pallas_call(
        keep,
        out_shape=shapes,
        in_specs=[vmem] * 3,
        out_specs=(vmem,) * 3,
        compiler_params=pltpu.CompilerParams(vmem_limit_bytes=4 * 1024 * 1024),
    )(*results)
    return act, bgrad, tgrad[None, None]


def solution(mesh):
    in_specs = (
        P(("grp", "shard"), None),
        P(("grp", "shard"), None, None),
        P(),
        P(None, "shard", None),
        P(),
        P(),
        P(("grp", "shard"), None),
    )
    out_specs = (
        P(("grp", "shard"), None),
        P(("grp", "shard"), None),
        P(None, "shard", "grp", None),
    )
    return jax.shard_map(
        on_device, mesh=mesh, in_specs=in_specs, out_specs=out_specs, check_vma=False
    )
```

```python
import jax
import jax.numpy as jnp
from jax import lax
from jax.experimental import pallas as pl
from jax.experimental.pallas import tpu as pltpu
from jax.sharding import PartitionSpec as P

HOT = 64
WIN = 328
NX, NZ, NC = 4, 4, 2
ZH, NY = 3, 8
CHIPS = NX * NZ
GROUPS = ZH * NY
B = 128
D = 128
OWN = GROUPS * HOT
ROWS = NC * OWN
PAD = WIN + HOT
OUT_ROWS = 336
F32, BF16, I32 = jnp.float32, jnp.bfloat16, jnp.int32
MESH = pl.DeviceIdType.MESH


def split_bf16(value):
    high = value.astype(BF16)
    return high, (value - high.astype(F32)).astype(BF16)


def kernel(
    bottom_hbm, lookups_hbm, pairs_hbm, starts_ref, tables_ref, dense_hbm, cot_hbm,
    act_ref, bgrad_ref, tgrad_ref,
    bottom_ref, lookups_ref, pairs_ref, dense_ref, cot_ref, start_of, win, hot, hot_t, idxs, et_a, et_b, part, rx, qz, zr, vs, pgs, grads, pre_dense, lsend, lrecv, outb, grecv, place_hot,
    local_sem, hot_sem, idx_send, idx_recv, vz_send, vz_recv, far_send, far_recv, vx_send, vx_recv,
    rs_send, rs_recv, z_send, z_recv, pg_send, pg_recv, l_send, l_recv, g_send, g_recv,
):
    g = lax.axis_index("grp")
    s = lax.axis_index("shard")
    zh, y = g // NY, g % NY
    et = (et_a, et_b)
    c = s % NC
    chip = s // NC
    x, z = chip // NZ, chip % NZ

    def at(chip_to):
        return (g, chip_to * NC + c)

    right = at((x + 1) % NX * NZ + z)
    left = at((x + NX - 1) % NX * NZ + z)
    partner = (g, chip * NC + (1 - c))

    def remote(src, dst, send, recv, to):
        return pltpu.make_async_remote_copy(
            src_ref=src, dst_ref=dst, send_sem=send, recv_sem=recv, device_id=to, device_id_type=MESH
        )

    first = (s * GROUPS // 128 - s // 27) * 128
    starts_in = pltpu.make_async_copy(starts_ref.at[:, pl.ds(pl.multiple_of(first, 128), 256)], start_of, local_sem.at[2])
    whole = pltpu.make_async_copy(tables_ref, win.at[:, pl.ds(0, WIN)], local_sem.at[0])
    again = pltpu.make_async_copy(tables_ref.at[:, pl.ds(0, HOT)], win.at[:, pl.ds(WIN, HOT)], local_sem.at[1])
    dense_in = pltpu.make_async_copy(dense_hbm, dense_ref, local_sem.at[3])
    cot_in = pltpu.make_async_copy(cot_hbm, cot_ref, local_sem.at[4])
    lookups_in = pltpu.make_async_copy(lookups_hbm, lookups_ref, local_sem.at[5])
    bottom_in = pltpu.make_async_copy(bottom_hbm, bottom_ref, local_sem.at[6])
    pairs_in = pltpu.make_async_copy(pairs_hbm, pairs_ref, local_sem.at[7])
    for copy in (lookups_in, bottom_in, starts_in, whole, again, dense_in, cot_in, pairs_in):
        copy.start()

    barrier = pltpu.get_barrier_semaphore()
    pl.semaphore_signal(barrier, inc=1, device_id=partner, device_id_type=MESH)
    for o in range(1, CHIPS):
        pl.semaphore_signal(barrier, inc=1, device_id=at((chip + o) % CHIPS), device_id_type=MESH)
    for o in range(1, GROUPS):
        pl.semaphore_signal(barrier, inc=1, device_id=((g + o) % GROUPS, s), device_id_type=MESH)

    lookups_in.wait()
    picked = lookups_ref[...]
    window = ((picked.astype(F32) + 0.5) * (1.0 / WIN)).astype(I32)
    hot_index = picked - window * (WIN - HOT)
    counts = jnp.zeros((4, B), I32)
    for k in range(4):
        counts = counts + jnp.where(hot_index == hot_index[k : k + 1], 1, 0)
    idxs[chip, 0:4] = hot_index
    idxs[chip, 4:8] = counts
    bottom_in.wait()
    vs[x, z] = bottom_ref[...].astype(F32)
    pl.semaphore_wait(barrier, 1 + CHIPS - 1 + GROUPS - 1)

    idx_out = [
        remote(idxs.at[chip], idxs.at[chip], idx_send.at[o - 1], idx_recv.at[chip], at((chip + o) % CHIPS))
        for o in range(1, CHIPS)
    ]
    for copy in idx_out:
        copy.start()
    vz_out = [
        remote(vs.at[x, z], vs.at[x, z], vz_send.at[o - 1], vz_recv.at[z], at(x * NZ + (z + o) % NZ))
        for o in range(1, NZ)
    ]
    for copy in vz_out:
        copy.start()
    x_far = (x + 2) % NX
    far_out = remote(vs.at[x, z], vs.at[x, z], far_send.at[NZ - 1], far_recv.at[z], at(x_far * NZ + z))
    far_out.start()
    far_on = [
        remote(vs.at[x_far, z], vs.at[x_far, z], far_send.at[o - 1], far_recv.at[z], at(x * NZ + (z + o) % NZ))
        for o in range(1, NZ)
    ]
    starts_in.wait()
    whole.wait()
    again.wait()
    for w in range(GROUPS):
        hot[pl.ds(c * OWN + w * HOT, HOT)] = win[w, pl.ds(start_of[g, s * GROUPS - first + w], HOT), :]
    mine = hot.at[pl.ds(c * OWN, OWN)]
    hot_out = remote(mine, mine, hot_sem.at[0], hot_sem.at[1], partner)
    hot_out.start()

    def turn_hot(half):
        def step(i, carry):
            at_row = pl.multiple_of(half * OWN + i * 128, 128)
            tile = hot[pl.ds(at_row, 128), :].T
            high, low = split_bf16(tile)
            hot_t[half * GROUPS // 2 + i, 0:D] = high
            hot_t[half * GROUPS // 2 + i, D:] = low
            return carry

        lax.fori_loop(0, OWN // 128, step, 0, unroll=4)

    turn_hot(c)
    dense_in.wait()
    pre_dense[...] = jnp.dot(bottom_ref[...], dense_ref[...], preferred_element_type=F32)
    hot_out.wait_recv()
    turn_hot(1 - c)

    def await_idx(k):
        remote(idxs.at[k], idxs.at[k], idx_send.at[0], idx_recv.at[k], left).wait_recv()

    for o in range(1, NZ):
        await_idx(x * NZ + (z + o) % NZ)

    row_iota = lax.broadcasted_iota(I32, (256, B), 0).astype(F32).astype(BF16)

    rs_to = {0: right, 1: left, 2: left, 3: right, 4: right, 5: left}
    rs_out = {p: remote(part.at[p], rx.at[p], rs_send.at[p], rs_recv.at[p], to) for p, to in rs_to.items()}

    def x_of(h, q):
        return (x + (2 + h + h // 2 * (2 * h - 3)) * (1 + 2 * q)) % NX

    def turn_of(xx, q):
        m = ((xx - x + NX) * (1 + 2 * q) + 2) % NX
        return m + m // 2 * (5 - 2 * m)

    def build(h, q):
        xx = x_of(h, q)
        for b in range(2):
            rows = idxs[xx * NZ + 2 * q + b]
            local = rows[0:4] - chip * ROWS
            counts = rows[4:8].astype(F32).astype(BF16)
            for j in range(ROWS // 256):
                near = jnp.clip(local - j * 256, -1, 256).astype(F32).astype(BF16)
                tile = jnp.zeros((256, B), BF16)
                for k in range(4):
                    tile = jnp.where(row_iota == near[k : k + 1], counts[k : k + 1], tile)
                et[q][2 * h + b, j] = tile

    def pool(h, q):
        both = jnp.dot(
            jnp.concatenate([hot_t[i] for i in range(ROWS // 128)], axis=1),
            jnp.concatenate([et[q][2 * h + b].reshape(ROWS, B) for b in range(2)], axis=1),
            preferred_element_type=F32,
        )
        summed = both[0:D] + both[D:]
        part[2 * h + q, 0] = summed[:, 0:B]
        part[2 * h + q, 1] = summed[:, B:]

    def pass_on(h, q):
        for k in rs_out:
            if k % 2 == q:

                @pl.when(h == k // 2)
                def _():
                    if k >= 4:
                        rs_out[k - 4].wait_recv()
                        part[k] = part[k] + rx[k - 4]
                    rs_out[k].start()
                    if k == 0:
                        remote(vs.at[x_far, z], vs.at[x_far, z], far_send.at[0], far_recv.at[z], left).wait_recv()
                        for copy in far_on:
                            copy.start()

    v_right = remote(vs.at[x], vs.at[x], vx_send.at[0], vx_recv.at[0], right)
    v_left = remote(vs.at[x], vs.at[x], vx_send.at[1], vx_recv.at[1], left)

    for b in range(2):
        await_idx(x_far * NZ + b)
    build(0, 0)

    def pool_step(h, carry):
        @pl.when(h < 3)
        def _():
            for b in range(2):
                await_idx(x_of(h, 1) * NZ + 2 + b)

        build(h, 1)
        pool(h, 0)
        pass_on(h, 0)

        @pl.when(h < 2)
        def _():
            for b in range(2):
                await_idx(x_of(h + 1, 0) * NZ + b)

        build((h + 1) % 4, 0)
        pool(h, 1)
        pass_on(h, 1)
        return carry

    lax.fori_loop(0, 4, pool_step, 0)

    for o in range(1, NZ):
        k = (z + o) % NZ
        remote(vs.at[x, k], vs.at[x, k], vz_send.at[o - 1], vz_recv.at[k], left).wait_recv()
    v_right.start()
    v_left.start()

    for q in range(2):
        a, b = (2, 4) if q == 0 else (3, 5)
        rs_out[a].wait_recv()
        rs_out[b].wait_recv()
        qz[pl.ds(2 * q, 2)] = part[6 + q] + rx[a] + rx[b]
        for k in (2 * q, 2 * q + 1):

            @pl.when(z != k)
            def _():
                remote(qz.at[k], zr.at[z], z_send.at[k], z_recv.at[z], at(x * NZ + k)).start()

    place_iota = lax.broadcasted_iota(I32, (OUT_ROWS, B), 0)
    lane = lax.broadcasted_iota(I32, (1, B), 1)
    column = s * GROUPS - first + g
    for i in range(OWN // B):
        place = lane % HOT + jnp.where(lane < HOT, start_of[2 * i, column], start_of[2 * i + 1, column])
        place = jnp.where(place >= WIN, place - WIN, place)
        place_hot[i] = jnp.where(place_iota == place, 1.0, 0.0).astype(BF16)

    pooled_t = qz[z]
    for o in range(1, NZ):
        k = (z + o) % NZ
        remote(qz.at[k], zr.at[k], z_send.at[0], z_recv.at[k], left).wait_recv()
        pooled_t = pooled_t + zr[k]
    pooled = pooled_t.T

    v0 = bottom_ref[...].astype(F32)
    cot_in.wait()
    pairs_in.wait()
    pair_dots = jnp.sum(v0 * pooled, axis=1, keepdims=True)
    preact = pre_dense[...] + pair_dots * pairs_ref[...]
    gate = jax.nn.sigmoid(preact)
    pre_grad = cot_ref[...] * gate * (1.0 + preact * (1.0 - gate))
    pair_grad = jnp.sum(pre_grad * pairs_ref[...], axis=1, keepdims=True)
    pgs[chip] = jnp.broadcast_to(pair_grad, (B, B)).T[0:8]
    pg_out = [
        remote(pgs.at[chip], pgs.at[chip], pg_send.at[o - 1], pg_recv.at[chip], at((chip + o) % CHIPS))
        for o in range(1, CHIPS)
    ]
    for copy in pg_out:
        copy.start()
    act_ref[...] = (preact * gate).astype(BF16)
    bgrad_ref[...] = (
        lax.dot_general(
            pre_grad.astype(BF16), dense_ref[...], (((1,), (1,)), ((), ())), preferred_element_type=F32
        )
        + pair_grad * pooled
    )

    v_right.wait_recv()
    v_left.wait_recv()
    for o in range(1, NZ):
        k = (z + o) % NZ
        remote(vs.at[x_far, k], vs.at[x_far, k], far_send.at[0], far_recv.at[k], left).wait_recv()
    for o in range(1, CHIPS):
        k = (chip + o) % CHIPS
        remote(pgs.at[k], pgs.at[k], pg_send.at[o - 1], pg_recv.at[k], left).wait_recv()
    columns = pgs[...].reshape(CHIPS * 8, B).T
    for i in range(CHIPS):
        xi, zi = i // NZ, i % NZ
        q = zi // 2
        slot = q * 8 + 2 * turn_of(xi, q) + zi % 2
        high, low = split_bf16(vs[xi, zi] * columns[:, 8 * i : 8 * i + 1])
        grads[0, slot] = high
        grads[1, slot] = low

    parts = [(zh + 1 + z // 2) % ZH, (zh + 2 + 2 * (z // 2)) % ZH, zh]

    def row_grads(half, i):
        rows = [
            jnp.concatenate([et[k // 8][k % 8, half * (OWN // 256) + parts[i] * 2 + block] for k in range(CHIPS)], axis=1)
            for block in range(2)
        ]
        right_side = jnp.concatenate([grads[k].reshape(CHIPS * B, D) for k in range(2)], axis=1)
        both = jnp.dot(jnp.concatenate(rows, axis=0), right_side, preferred_element_type=F32)
        return both[:, 0:D] + both[:, D:]

    l_out = [remote(lsend.at[i], lrecv.at[i], l_send.at[i], l_recv.at[i], partner) for i in range(3)]
    g_out = []
    for i in range(3):
        lsend[i] = row_grads(1 - c, i)
        l_out[i].start()
        total = row_grads(c, i)
        l_out[i].wait_recv()
        outb[i] = (total + lrecv[i]).reshape(NY, HOT, D)
        for o in (4, 3, 5, 2, 6, 1, 7, 0):
            if i == 2 and o == 0:
                continue
            k = (y + o) % NY
            copy = remote(outb.at[i, k], grecv.at[g], g_send.at[len(g_out)], g_recv.at[g], (parts[i] * NY + k, s))
            copy.start()
            g_out.append(copy)
    grecv[g] = outb[2, y]
    for o in range(1, GROUPS):
        k = (g + o) % GROUPS
        remote(grecv.at[k], grecv.at[k], g_send.at[0], g_recv.at[k], left).wait_recv()
    high, low = split_bf16(grecv[...].reshape(OWN, D))
    both = jnp.dot(
        jnp.concatenate([place_hot[i] for i in range(OWN // B)], axis=1),
        jnp.concatenate([high, low], axis=1),
        preferred_element_type=F32,
    )
    tgrad_ref[...] = (both[:, 0:D] + both[:, D:])[0:WIN]

    hot_out.wait_send()
    for copy in (*idx_out, *vz_out, *rs_out.values(), v_right, v_left, far_out, *far_on):
        copy.wait_send()
    for copy in (*pg_out, *l_out, *g_out):
        copy.wait_send()
    for o in range(1, NZ):
        k = (z + o) % NZ
        remote(qz.at[k], zr.at[z], z_send.at[k], z_recv.at[z], at(x * NZ + k)).wait_send()


def keep(*refs):
    for source, target in zip(refs[:3], refs[3:]):
        target[...] = source[...]


def on_device(bottom_out, lookups, starts, tables, top_dense, top_pairs, cotangent):
    vmem = pl.BlockSpec(memory_space=pltpu.VMEM)
    dma = pltpu.SemaphoreType.DMA
    hbm = pl.BlockSpec(memory_space=pltpu.HBM)
    shapes = (
        jax.ShapeDtypeStruct((B, 1024), BF16),
        jax.ShapeDtypeStruct((B, D), F32),
        jax.ShapeDtypeStruct((WIN, D), F32),
    )
    operands = (
        bottom_out, lookups[:, 0, :].T, top_pairs, starts, tables.reshape(GROUPS, WIN, D), top_dense, cotangent,
    )
    results = pl.pallas_call(
        kernel,
        out_shape=shapes,
        in_specs=[hbm] * 7,
        out_specs=(vmem, vmem, vmem),
        scratch_shapes=[
            pltpu.VMEM((B, D), BF16),
            pltpu.VMEM((4, B), I32),
            pltpu.VMEM((1, 1024), F32),
            pltpu.VMEM((D, 1024), BF16),
            pltpu.VMEM((B, 1024), F32),
            pltpu.SMEM((GROUPS, 256), I32),
            pltpu.VMEM((GROUPS, PAD, D), F32),
            pltpu.VMEM((ROWS, D), F32),
            pltpu.VMEM((ROWS // 128, 2 * D, 128), BF16),
            pltpu.VMEM((CHIPS, 8, B), I32),
            pltpu.VMEM((CHIPS // 2, ROWS // 256, 256, B), BF16),
            pltpu.VMEM((CHIPS // 2, ROWS // 256, 256, B), BF16),
            pltpu.VMEM((8, 2, D, B), F32),
            pltpu.VMEM((6, 2, D, B), F32),
            pltpu.VMEM((NZ, D, B), F32),
            pltpu.VMEM((NZ, D, B), F32),
            pltpu.VMEM((NX, NZ, B, D), F32),
            pltpu.VMEM((CHIPS, 8, B), F32),
            pltpu.VMEM((2, CHIPS, B, D), BF16),
            pltpu.VMEM((B, 1024), F32),
            pltpu.VMEM((ZH, NY * HOT, D), F32),
            pltpu.VMEM((ZH, NY * HOT, D), F32),
            pltpu.VMEM((ZH, NY, HOT, D), F32),
            pltpu.VMEM((GROUPS, HOT, D), F32),
            pltpu.VMEM((OWN // B, OUT_ROWS, B), BF16),
            dma((8,)), dma((2,)), dma((CHIPS - 1,)), dma((CHIPS,)), dma((NZ - 1,)), dma((NZ,)), dma((NZ,)), dma((NZ,)), dma((2,)), dma((2,)),
            dma((6,)), dma((6,)), dma((NZ,)), dma((NZ,)), dma((CHIPS - 1,)), dma((CHIPS,)),
            dma((ZH,)), dma((ZH,)), dma((GROUPS,)), dma((GROUPS,)),
        ],
        compiler_params=pltpu.CompilerParams(
            collective_id=0, has_side_effects=True, vmem_limit_bytes=38 * 1024 * 1024
        ),
    )(
        *(pltpu.with_memory_space_constraint(value, pltpu.HBM) for value in operands)
    )
    act, bgrad, tgrad = pl.pallas_call(
        keep,
        out_shape=shapes,
        in_specs=[vmem] * 3,
        out_specs=(vmem,) * 3,
        compiler_params=pltpu.CompilerParams(vmem_limit_bytes=4 * 1024 * 1024),
    )(*results)
    return act, bgrad, tgrad[None, None]


def solution(mesh):
    in_specs = (
        P(("grp", "shard"), None),
        P(("grp", "shard"), None, None),
        P(),
        P(None, "shard", None),
        P(),
        P(),
        P(("grp", "shard"), None),
    )
    out_specs = (
        P(("grp", "shard"), None),
        P(("grp", "shard"), None),
        P(None, "shard", "grp", None),
    )
    return jax.shard_map(
        on_device, mesh=mesh, in_specs=in_specs, out_specs=out_specs, check_vma=False
    )
```

```python
import jax
import jax.numpy as jnp
from jax import lax
from jax.experimental import pallas as pl
from jax.experimental.pallas import tpu as pltpu
from jax.sharding import PartitionSpec as P

HOT = 64
WIN = 328
NX, NZ, NC = 4, 4, 2
ZH, NY = 3, 8
CHIPS = NX * NZ
GROUPS = ZH * NY
B = 128
D = 128
OWN = GROUPS * HOT
ROWS = NC * OWN
PAD = WIN + HOT
OUT_ROWS = 336
F32, BF16, I32 = jnp.float32, jnp.bfloat16, jnp.int32
MESH = pl.DeviceIdType.MESH


def split_bf16(value):
    high = value.astype(BF16)
    return high, (value - high.astype(F32)).astype(BF16)


def kernel(
    bottom_hbm, lookups_hbm, pairs_hbm, starts_ref, tables_ref, dense_hbm, cot_hbm,
    act_ref, bgrad_ref, tgrad_ref,
    bottom_ref, lookups_ref, pairs_ref, dense_ref, cot_ref, start_of, win, hot, hot_t, idxs, et_a, et_b, part, rx, qz, zr, vs, pgs, grads, pre_dense, lsend, lrecv, outb, grecv, place_hot,
    local_sem, hot_sem, idx_send, idx_recv, vz_send, vz_recv, far_send, far_recv, vx_send, vx_recv,
    rs_send, rs_recv, z_send, z_recv, pg_send, pg_recv, l_send, l_recv, g_send, g_recv,
):
    g = lax.axis_index("grp")
    s = lax.axis_index("shard")
    zh, y = g // NY, g % NY
    et = (et_a, et_b)
    c = s % NC
    chip = s // NC
    x, z = chip // NZ, chip % NZ

    def at(chip_to):
        return (g, chip_to * NC + c)

    right = at((x + 1) % NX * NZ + z)
    left = at((x + NX - 1) % NX * NZ + z)
    partner = (g, chip * NC + (1 - c))

    def remote(src, dst, send, recv, to):
        return pltpu.make_async_remote_copy(
            src_ref=src, dst_ref=dst, send_sem=send, recv_sem=recv, device_id=to, device_id_type=MESH
        )

    first = (s * GROUPS // 128 - s // 27) * 128
    starts_in = pltpu.make_async_copy(starts_ref.at[:, pl.ds(pl.multiple_of(first, 128), 256)], start_of, local_sem.at[2])
    whole = pltpu.make_async_copy(tables_ref, win.at[:, pl.ds(0, WIN)], local_sem.at[0])
    again = pltpu.make_async_copy(tables_ref.at[:, pl.ds(0, HOT)], win.at[:, pl.ds(WIN, HOT)], local_sem.at[1])
    dense_in = pltpu.make_async_copy(dense_hbm, dense_ref, local_sem.at[3])
    cot_in = pltpu.make_async_copy(cot_hbm, cot_ref, local_sem.at[4])
    lookups_in = pltpu.make_async_copy(lookups_hbm, lookups_ref, local_sem.at[5])
    bottom_in = pltpu.make_async_copy(bottom_hbm, bottom_ref, local_sem.at[6])
    pairs_in = pltpu.make_async_copy(pairs_hbm, pairs_ref, local_sem.at[7])
    for copy in (lookups_in, bottom_in, starts_in, whole, again, dense_in, cot_in, pairs_in):
        copy.start()

    barrier = pltpu.get_barrier_semaphore()
    pl.semaphore_signal(barrier, inc=1, device_id=partner, device_id_type=MESH)
    for o in range(1, CHIPS):
        pl.semaphore_signal(barrier, inc=1, device_id=at((chip + o) % CHIPS), device_id_type=MESH)
    for o in range(1, GROUPS):
        pl.semaphore_signal(barrier, inc=1, device_id=((g + o) % GROUPS, s), device_id_type=MESH)

    lookups_in.wait()
    picked = lookups_ref[...]
    window = ((picked.astype(F32) + 0.5) * (1.0 / WIN)).astype(I32)
    hot_index = picked - window * (WIN - HOT)
    counts = jnp.zeros((4, B), I32)
    for k in range(4):
        counts = counts + jnp.where(hot_index == hot_index[k : k + 1], 1, 0)
    idxs[chip, 0:4] = hot_index
    idxs[chip, 4:8] = counts
    bottom_in.wait()
    vs[x, z] = bottom_ref[...].astype(F32)
    pl.semaphore_wait(barrier, 1 + CHIPS - 1 + GROUPS - 1)

    idx_out = [
        remote(idxs.at[chip], idxs.at[chip], idx_send.at[o - 1], idx_recv.at[chip], at((chip + o) % CHIPS))
        for o in range(1, CHIPS)
    ]
    for copy in idx_out:
        copy.start()
    vz_out = [
        remote(vs.at[x, z], vs.at[x, z], vz_send.at[o - 1], vz_recv.at[z], at(x * NZ + (z + o) % NZ))
        for o in range(1, NZ)
    ]
    for copy in vz_out:
        copy.start()
    x_far = (x + 2) % NX
    far_out = remote(vs.at[x, z], vs.at[x, z], far_send.at[NZ - 1], far_recv.at[z], at(x_far * NZ + z))
    far_out.start()
    far_on = [
        remote(vs.at[x_far, z], vs.at[x_far, z], far_send.at[o - 1], far_recv.at[z], at(x * NZ + (z + o) % NZ))
        for o in range(1, NZ)
    ]
    starts_in.wait()
    whole.wait()
    again.wait()
    for w in range(GROUPS):
        hot[pl.ds(c * OWN + w * HOT, HOT)] = win[w, pl.ds(start_of[g, s * GROUPS - first + w], HOT), :]
    mine = hot.at[pl.ds(c * OWN, OWN)]
    hot_out = remote(mine, mine, hot_sem.at[0], hot_sem.at[1], partner)
    hot_out.start()

    def turn_hot(half):
        def step(i, carry):
            at_row = pl.multiple_of(half * OWN + i * 128, 128)
            tile = hot[pl.ds(at_row, 128), :].T
            high, low = split_bf16(tile)
            hot_t[half * GROUPS // 2 + i, 0:D] = high
            hot_t[half * GROUPS // 2 + i, D:] = low
            return carry

        lax.fori_loop(0, OWN // 128, step, 0, unroll=4)

    turn_hot(c)
    dense_in.wait()
    pre_dense[...] = jnp.dot(bottom_ref[...], dense_ref[...], preferred_element_type=F32)
    hot_out.wait_recv()
    turn_hot(1 - c)

    def await_idx(k):
        remote(idxs.at[k], idxs.at[k], idx_send.at[0], idx_recv.at[k], left).wait_recv()

    for o in range(1, NZ):
        await_idx(x * NZ + (z + o) % NZ)

    row_iota = lax.broadcasted_iota(I32, (256, B), 0).astype(F32).astype(BF16)

    rs_to = {0: right, 1: left, 2: left, 3: right, 4: right, 5: left}
    rs_out = {p: remote(part.at[p], rx.at[p], rs_send.at[p], rs_recv.at[p], to) for p, to in rs_to.items()}

    def x_of(h, q):
        return (x + (2 + h + h // 2 * (2 * h - 3)) * (1 + 2 * q)) % NX

    def turn_of(xx, q):
        m = ((xx - x + NX) * (1 + 2 * q) + 2) % NX
        return m + m // 2 * (5 - 2 * m)

    def build(h, q):
        xx = x_of(h, q)
        for b in range(2):
            rows = idxs[xx * NZ + 2 * q + b]
            local = rows[0:4] - chip * ROWS
            counts = rows[4:8].astype(F32).astype(BF16)
            for j in range(ROWS // 256):
                near = jnp.clip(local - j * 256, -1, 256).astype(F32).astype(BF16)
                tile = jnp.zeros((256, B), BF16)
                for k in range(4):
                    tile = jnp.where(row_iota == near[k : k + 1], counts[k : k + 1], tile)
                et[q][2 * h + b, j] = tile

    def pool(h, q):
        both = jnp.dot(
            jnp.concatenate([hot_t[i] for i in range(ROWS // 128)], axis=1),
            jnp.concatenate([et[q][2 * h + b].reshape(ROWS, B) for b in range(2)], axis=1),
            preferred_element_type=F32,
        )
        summed = both[0:D] + both[D:]
        part[2 * h + q, 0] = summed[:, 0:B]
        part[2 * h + q, 1] = summed[:, B:]

    def pass_on(h, q):
        for k in rs_out:
            if k % 2 == q:

                @pl.when(h == k // 2)
                def _():
                    if k >= 4:
                        rs_out[k - 4].wait_recv()
                        part[k] = part[k] + rx[k - 4]
                    rs_out[k].start()
                    if k == 0:
                        remote(vs.at[x_far, z], vs.at[x_far, z], far_send.at[0], far_recv.at[z], left).wait_recv()
                        for copy in far_on:
                            copy.start()

    v_right = remote(vs.at[x], vs.at[x], vx_send.at[0], vx_recv.at[0], right)
    v_left = remote(vs.at[x], vs.at[x], vx_send.at[1], vx_recv.at[1], left)

    for b in range(2):
        await_idx(x_far * NZ + b)
    build(0, 0)

    def pool_step(h, carry):
        @pl.when(h < 3)
        def _():
            for b in range(2):
                await_idx(x_of(h, 1) * NZ + 2 + b)

        build(h, 1)
        pool(h, 0)
        pass_on(h, 0)

        @pl.when(h < 2)
        def _():
            for b in range(2):
                await_idx(x_of(h + 1, 0) * NZ + b)

        build((h + 1) % 4, 0)
        pool(h, 1)
        pass_on(h, 1)
        return carry

    lax.fori_loop(0, 4, pool_step, 0)

    for o in range(1, NZ):
        k = (z + o) % NZ
        remote(vs.at[x, k], vs.at[x, k], vz_send.at[o - 1], vz_recv.at[k], left).wait_recv()
    v_right.start()
    v_left.start()

    for q in range(2):
        a, b = (2, 4) if q == 0 else (3, 5)
        rs_out[a].wait_recv()
        rs_out[b].wait_recv()
        qz[pl.ds(2 * q, 2)] = part[6 + q] + rx[a] + rx[b]
        for k in (2 * q, 2 * q + 1):

            @pl.when(z != k)
            def _():
                remote(qz.at[k], zr.at[z], z_send.at[k], z_recv.at[z], at(x * NZ + k)).start()

    place_iota = lax.broadcasted_iota(I32, (OUT_ROWS, B), 0)
    lane = lax.broadcasted_iota(I32, (1, B), 1)
    column = s * GROUPS - first + g
    for i in range(OWN // B):
        place = lane % HOT + jnp.where(lane < HOT, start_of[2 * i, column], start_of[2 * i + 1, column])
        place = jnp.where(place >= WIN, place - WIN, place)
        place_hot[i] = jnp.where(place_iota == place, 1.0, 0.0).astype(BF16)

    pooled_t = qz[z]
    for o in range(1, NZ):
        k = (z + o) % NZ
        remote(qz.at[k], zr.at[k], z_send.at[0], z_recv.at[k], left).wait_recv()
        pooled_t = pooled_t + zr[k]
    pooled = pooled_t.T

    v0 = bottom_ref[...].astype(F32)
    cot_in.wait()
    pairs_in.wait()
    pair_dots = jnp.sum(v0 * pooled, axis=1, keepdims=True)
    preact = pre_dense[...] + pair_dots * pairs_ref[...]
    gate = jax.nn.sigmoid(preact)
    pre_grad = cot_ref[...] * gate * (1.0 + preact * (1.0 - gate))
    pair_grad = jnp.sum(pre_grad * pairs_ref[...], axis=1, keepdims=True)
    pgs[chip] = jnp.broadcast_to(pair_grad, (B, B)).T[0:8]
    pg_out = [
        remote(pgs.at[chip], pgs.at[chip], pg_send.at[o - 1], pg_recv.at[chip], at((chip + o) % CHIPS))
        for o in range(1, CHIPS)
    ]
    for copy in pg_out:
        copy.start()
    act_ref[...] = (preact * gate).astype(BF16)
    bgrad_ref[...] = (
        lax.dot_general(
            pre_grad.astype(BF16), dense_ref[...], (((1,), (1,)), ((), ())), preferred_element_type=F32
        )
        + pair_grad * pooled
    )

    v_right.wait_recv()
    v_left.wait_recv()
    for o in range(1, NZ):
        k = (z + o) % NZ
        remote(vs.at[x_far, k], vs.at[x_far, k], far_send.at[0], far_recv.at[k], left).wait_recv()
    for o in range(1, CHIPS):
        k = (chip + o) % CHIPS
        remote(pgs.at[k], pgs.at[k], pg_send.at[o - 1], pg_recv.at[k], left).wait_recv()
    columns = pgs[...].reshape(CHIPS * 8, B).T
    for i in range(CHIPS):
        xi, zi = i // NZ, i % NZ
        q = zi // 2
        slot = q * 8 + 2 * turn_of(xi, q) + zi % 2
        high, low = split_bf16(vs[xi, zi] * columns[:, 8 * i : 8 * i + 1])
        grads[0, slot] = high
        grads[1, slot] = low

    parts = [(zh + 1 + z // 2) % ZH, (zh + 2 + 2 * (z // 2)) % ZH, zh]

    def row_grads(half, i):
        rows = [
            jnp.concatenate([et[k // 8][k % 8, half * (OWN // 256) + parts[i] * 2 + block] for k in range(CHIPS)], axis=1)
            for block in range(2)
        ]
        right_side = jnp.concatenate([grads[k].reshape(CHIPS * B, D) for k in range(2)], axis=1)
        both = jnp.dot(jnp.concatenate(rows, axis=0), right_side, preferred_element_type=F32)
        return both[:, 0:D] + both[:, D:]

    l_out = [remote(lsend.at[i], lrecv.at[i], l_send.at[i], l_recv.at[i], partner) for i in range(3)]
    g_out = []
    for i in range(3):
        lsend[i] = row_grads(1 - c, i)
        l_out[i].start()
        total = row_grads(c, i)
        l_out[i].wait_recv()
        outb[i] = (total + lrecv[i]).reshape(NY, HOT, D)
        for o in (1, 7, 2, 6, 3, 5, 4, 0):
            if i == 2 and o == 0:
                continue
            k = (y + o) % NY
            copy = remote(outb.at[i, k], grecv.at[g], g_send.at[len(g_out)], g_recv.at[g], (parts[i] * NY + k, s))
            copy.start()
            g_out.append(copy)
    grecv[g] = outb[2, y]
    for o in range(1, GROUPS):
        k = (g + o) % GROUPS
        remote(grecv.at[k], grecv.at[k], g_send.at[0], g_recv.at[k], left).wait_recv()
    high, low = split_bf16(grecv[...].reshape(OWN, D))
    both = jnp.dot(
        jnp.concatenate([place_hot[i] for i in range(OWN // B)], axis=1),
        jnp.concatenate([high, low], axis=1),
        preferred_element_type=F32,
    )
    tgrad_ref[...] = (both[:, 0:D] + both[:, D:])[0:WIN]

    hot_out.wait_send()
    for copy in (*idx_out, *vz_out, *rs_out.values(), v_right, v_left, far_out, *far_on):
        copy.wait_send()
    for copy in (*pg_out, *l_out, *g_out):
        copy.wait_send()
    for o in range(1, NZ):
        k = (z + o) % NZ
        remote(qz.at[k], zr.at[z], z_send.at[k], z_recv.at[z], at(x * NZ + k)).wait_send()


def keep(*refs):
    for source, target in zip(refs[:3], refs[3:]):
        target[...] = source[...]


def on_device(bottom_out, lookups, starts, tables, top_dense, top_pairs, cotangent):
    vmem = pl.BlockSpec(memory_space=pltpu.VMEM)
    dma = pltpu.SemaphoreType.DMA
    hbm = pl.BlockSpec(memory_space=pltpu.HBM)
    shapes = (
        jax.ShapeDtypeStruct((B, 1024), BF16),
        jax.ShapeDtypeStruct((B, D), F32),
        jax.ShapeDtypeStruct((WIN, D), F32),
    )
    operands = (
        bottom_out, lookups[:, 0, :].T, top_pairs, starts, tables.reshape(GROUPS, WIN, D), top_dense, cotangent,
    )
    results = pl.pallas_call(
        kernel,
        out_shape=shapes,
        in_specs=[hbm] * 7,
        out_specs=(vmem, vmem, vmem),
        scratch_shapes=[
            pltpu.VMEM((B, D), BF16),
            pltpu.VMEM((4, B), I32),
            pltpu.VMEM((1, 1024), F32),
            pltpu.VMEM((D, 1024), BF16),
            pltpu.VMEM((B, 1024), F32),
            pltpu.SMEM((GROUPS, 256), I32),
            pltpu.VMEM((GROUPS, PAD, D), F32),
            pltpu.VMEM((ROWS, D), F32),
            pltpu.VMEM((ROWS // 128, 2 * D, 128), BF16),
            pltpu.VMEM((CHIPS, 8, B), I32),
            pltpu.VMEM((CHIPS // 2, ROWS // 256, 256, B), BF16),
            pltpu.VMEM((CHIPS // 2, ROWS // 256, 256, B), BF16),
            pltpu.VMEM((8, 2, D, B), F32),
            pltpu.VMEM((6, 2, D, B), F32),
            pltpu.VMEM((NZ, D, B), F32),
            pltpu.VMEM((NZ, D, B), F32),
            pltpu.VMEM((NX, NZ, B, D), F32),
            pltpu.VMEM((CHIPS, 8, B), F32),
            pltpu.VMEM((2, CHIPS, B, D), BF16),
            pltpu.VMEM((B, 1024), F32),
            pltpu.VMEM((ZH, NY * HOT, D), F32),
            pltpu.VMEM((ZH, NY * HOT, D), F32),
            pltpu.VMEM((ZH, NY, HOT, D), F32),
            pltpu.VMEM((GROUPS, HOT, D), F32),
            pltpu.VMEM((OWN // B, OUT_ROWS, B), BF16),
            dma((8,)), dma((2,)), dma((CHIPS - 1,)), dma((CHIPS,)), dma((NZ - 1,)), dma((NZ,)), dma((NZ,)), dma((NZ,)), dma((2,)), dma((2,)),
            dma((6,)), dma((6,)), dma((NZ,)), dma((NZ,)), dma((CHIPS - 1,)), dma((CHIPS,)),
            dma((ZH,)), dma((ZH,)), dma((GROUPS,)), dma((GROUPS,)),
        ],
        compiler_params=pltpu.CompilerParams(
            collective_id=0, has_side_effects=True, vmem_limit_bytes=38 * 1024 * 1024
        ),
    )(
        *(pltpu.with_memory_space_constraint(value, pltpu.HBM) for value in operands)
    )
    act, bgrad, tgrad = pl.pallas_call(
        keep,
        out_shape=shapes,
        in_specs=[vmem] * 3,
        out_specs=(vmem,) * 3,
        compiler_params=pltpu.CompilerParams(vmem_limit_bytes=4 * 1024 * 1024),
    )(*results)
    return act, bgrad, tgrad[None, None]


def solution(mesh):
    in_specs = (
        P(("grp", "shard"), None),
        P(("grp", "shard"), None, None),
        P(),
        P(None, "shard", None),
        P(),
        P(),
        P(("grp", "shard"), None),
    )
    out_specs = (
        P(("grp", "shard"), None),
        P(("grp", "shard"), None),
        P(None, "shard", "grp", None),
    )
    return jax.shard_map(
        on_device, mesh=mesh, in_specs=in_specs, out_specs=out_specs, check_vma=False
    )
```

```python
import jax
import jax.numpy as jnp
from jax import lax
from jax.experimental import pallas as pl
from jax.experimental.pallas import tpu as pltpu
from jax.sharding import PartitionSpec as P

HOT = 64
WIN = 328
NX, NZ, NC = 4, 4, 2
ZH, NY = 3, 8
CHIPS = NX * NZ
GROUPS = ZH * NY
B = 128
D = 128
OWN = GROUPS * HOT
ROWS = NC * OWN
PAD = WIN + HOT
OUT_ROWS = 336
F32, BF16, I32 = jnp.float32, jnp.bfloat16, jnp.int32
MESH = pl.DeviceIdType.MESH


def split_bf16(value):
    high = value.astype(BF16)
    return high, (value - high.astype(F32)).astype(BF16)


def kernel(
    bottom_hbm, lookups_hbm, pairs_hbm, starts_ref, tables_ref, dense_hbm, cot_hbm,
    act_ref, bgrad_ref, tgrad_ref,
    bottom_ref, lookups_ref, pairs_ref, dense_ref, cot_ref, start_of, win, hot, hot_t, idxs, et_a, et_b, part, rx, qz, zr, vs, pgs, grads, pre_dense, lsend, lrecv, outb, grecv, place_hot,
    local_sem, hot_sem, idx_send, idx_recv, vz_send, vz_recv, far_send, far_recv, vx_send, vx_recv,
    rs_send, rs_recv, z_send, z_recv, pg_send, pg_recv, l_send, l_recv, g_send, g_recv,
):
    g = lax.axis_index("grp")
    s = lax.axis_index("shard")
    zh, y = g // NY, g % NY
    et = (et_a, et_b)
    c = s % NC
    chip = s // NC
    x, z = chip // NZ, chip % NZ

    def at(chip_to):
        return (g, chip_to * NC + c)

    right = at((x + 1) % NX * NZ + z)
    left = at((x + NX - 1) % NX * NZ + z)
    partner = (g, chip * NC + (1 - c))

    def remote(src, dst, send, recv, to):
        return pltpu.make_async_remote_copy(
            src_ref=src, dst_ref=dst, send_sem=send, recv_sem=recv, device_id=to, device_id_type=MESH
        )

    first = (s * GROUPS // 128 - s // 27) * 128
    starts_in = pltpu.make_async_copy(starts_ref.at[:, pl.ds(pl.multiple_of(first, 128), 256)], start_of, local_sem.at[2])
    whole = pltpu.make_async_copy(tables_ref, win.at[:, pl.ds(0, WIN)], local_sem.at[0])
    again = pltpu.make_async_copy(tables_ref.at[:, pl.ds(0, HOT)], win.at[:, pl.ds(WIN, HOT)], local_sem.at[1])
    dense_in = pltpu.make_async_copy(dense_hbm, dense_ref, local_sem.at[3])
    cot_in = pltpu.make_async_copy(cot_hbm, cot_ref, local_sem.at[4])
    lookups_in = pltpu.make_async_copy(lookups_hbm, lookups_ref, local_sem.at[5])
    bottom_in = pltpu.make_async_copy(bottom_hbm, bottom_ref, local_sem.at[6])
    pairs_in = pltpu.make_async_copy(pairs_hbm, pairs_ref, local_sem.at[7])
    for copy in (lookups_in, bottom_in, starts_in, whole, again, dense_in, cot_in, pairs_in):
        copy.start()

    barrier = pltpu.get_barrier_semaphore()
    pl.semaphore_signal(barrier, inc=1, device_id=partner, device_id_type=MESH)
    for o in range(1, CHIPS):
        pl.semaphore_signal(barrier, inc=1, device_id=at((chip + o) % CHIPS), device_id_type=MESH)
    for o in range(1, GROUPS):
        pl.semaphore_signal(barrier, inc=1, device_id=((g + o) % GROUPS, s), device_id_type=MESH)

    lookups_in.wait()
    picked = lookups_ref[...]
    window = ((picked.astype(F32) + 0.5) * (1.0 / WIN)).astype(I32)
    hot_index = picked - window * (WIN - HOT)
    counts = jnp.zeros((4, B), I32)
    for k in range(4):
        counts = counts + jnp.where(hot_index == hot_index[k : k + 1], 1, 0)
    idxs[chip, 0:4] = hot_index
    idxs[chip, 4:8] = counts
    bottom_in.wait()
    vs[x, z] = bottom_ref[...].astype(F32)
    pl.semaphore_wait(barrier, 1 + CHIPS - 1 + GROUPS - 1)

    idx_out = [
        remote(idxs.at[chip], idxs.at[chip], idx_send.at[o - 1], idx_recv.at[chip], at((chip + o) % CHIPS))
        for o in range(1, CHIPS)
    ]
    for copy in idx_out:
        copy.start()
    vz_out = [
        remote(vs.at[x, z], vs.at[x, z], vz_send.at[o - 1], vz_recv.at[z], at(x * NZ + (z + o) % NZ))
        for o in range(1, NZ)
    ]
    for copy in vz_out:
        copy.start()
    x_far = (x + 2) % NX
    far_out = remote(vs.at[x, z], vs.at[x, z], far_send.at[NZ - 1], far_recv.at[z], at(x_far * NZ + z))
    far_out.start()
    far_on = [
        remote(vs.at[x_far, z], vs.at[x_far, z], far_send.at[o - 1], far_recv.at[z], at(x * NZ + (z + o) % NZ))
        for o in range(1, NZ)
    ]
    starts_in.wait()
    whole.wait()
    again.wait()
    for w in range(GROUPS):
        hot[pl.ds(c * OWN + w * HOT, HOT)] = win[w, pl.ds(start_of[g, s * GROUPS - first + w], HOT), :]
    mine = hot.at[pl.ds(c * OWN, OWN)]
    hot_out = remote(mine, mine, hot_sem.at[0], hot_sem.at[1], partner)
    hot_out.start()

    def turn_hot(half):
        def step(i, carry):
            at_row = pl.multiple_of(half * OWN + i * 128, 128)
            tile = hot[pl.ds(at_row, 128), :].T
            high, low = split_bf16(tile)
            hot_t[half * GROUPS // 2 + i, 0:D] = high
            hot_t[half * GROUPS // 2 + i, D:] = low
            return carry

        lax.fori_loop(0, OWN // 128, step, 0, unroll=4)

    turn_hot(c)
    dense_in.wait()
    pre_dense[...] = jnp.dot(bottom_ref[...], dense_ref[...], preferred_element_type=F32)
    hot_out.wait_recv()
    turn_hot(1 - c)

    def await_idx(k):
        remote(idxs.at[k], idxs.at[k], idx_send.at[0], idx_recv.at[k], left).wait_recv()

    for o in range(1, NZ):
        await_idx(x * NZ + (z + o) % NZ)

    row_iota = lax.broadcasted_iota(I32, (256, B), 0).astype(F32).astype(BF16)

    rs_to = {0: right, 1: left, 2: left, 3: right, 4: right, 5: left}
    rs_out = {p: remote(part.at[p], rx.at[p], rs_send.at[p], rs_recv.at[p], to) for p, to in rs_to.items()}

    def x_of(h, q):
        return (x + (2 + h + h // 2 * (2 * h - 3)) * (1 + 2 * q)) % NX

    def turn_of(xx, q):
        m = ((xx - x + NX) * (1 + 2 * q) + 2) % NX
        return m + m // 2 * (5 - 2 * m)

    def build(h, q):
        xx = x_of(h, q)
        for b in range(2):
            rows = idxs[xx * NZ + 2 * q + b]
            local = rows[0:4] - chip * ROWS
            counts = rows[4:8].astype(F32).astype(BF16)
            for j in range(ROWS // 256):
                near = jnp.clip(local - j * 256, -1, 256).astype(F32).astype(BF16)
                tile = jnp.zeros((256, B), BF16)
                for k in range(4):
                    tile = jnp.where(row_iota == near[k : k + 1], counts[k : k + 1], tile)
                et[q][2 * h + b, j] = tile

    def pool(h, q):
        both = jnp.dot(
            jnp.concatenate([hot_t[i] for i in range(ROWS // 128)], axis=1),
            jnp.concatenate([et[q][2 * h + b].reshape(ROWS, B) for b in range(2)], axis=1),
            preferred_element_type=F32,
        )
        summed = both[0:D] + both[D:]
        part[2 * h + q, 0] = summed[:, 0:B]
        part[2 * h + q, 1] = summed[:, B:]

    def pass_on(h, q):
        for k in rs_out:
            if k % 2 == q:

                @pl.when(h == k // 2)
                def _():
                    if k >= 4:
                        rs_out[k - 4].wait_recv()
                        part[k] = part[k] + rx[k - 4]
                    rs_out[k].start()
                    if k == 0:
                        remote(vs.at[x_far, z], vs.at[x_far, z], far_send.at[0], far_recv.at[z], left).wait_recv()
                        for copy in far_on:
                            copy.start()

    v_right = remote(vs.at[x], vs.at[x], vx_send.at[0], vx_recv.at[0], right)
    v_left = remote(vs.at[x], vs.at[x], vx_send.at[1], vx_recv.at[1], left)

    for b in range(2):
        await_idx(x_far * NZ + b)
    build(0, 0)

    def pool_step(h, carry):
        @pl.when(h < 3)
        def _():
            for b in range(2):
                await_idx(x_of(h, 1) * NZ + 2 + b)

        build(h, 1)
        pool(h, 0)
        pass_on(h, 0)

        @pl.when(h < 2)
        def _():
            for b in range(2):
                await_idx(x_of(h + 1, 0) * NZ + b)

        build((h + 1) % 4, 0)
        pool(h, 1)
        pass_on(h, 1)
        return carry

    lax.fori_loop(0, 4, pool_step, 0)

    for o in range(1, NZ):
        k = (z + o) % NZ
        remote(vs.at[x, k], vs.at[x, k], vz_send.at[o - 1], vz_recv.at[k], left).wait_recv()
    v_right.start()
    v_left.start()

    for q in range(2):
        a, b = (2, 4) if q == 0 else (3, 5)
        rs_out[a].wait_recv()
        rs_out[b].wait_recv()
        qz[pl.ds(2 * q, 2)] = part[6 + q] + rx[a] + rx[b]
        for k in (2 * q, 2 * q + 1):

            @pl.when(z != k)
            def _():
                remote(qz.at[k], zr.at[z], z_send.at[k], z_recv.at[z], at(x * NZ + k)).start()

    place_iota = lax.broadcasted_iota(I32, (OUT_ROWS, B), 0)
    lane = lax.broadcasted_iota(I32, (1, B), 1)
    column = s * GROUPS - first + g
    for i in range(OWN // B):
        place = lane % HOT + jnp.where(lane < HOT, start_of[2 * i, column], start_of[2 * i + 1, column])
        place = jnp.where(place >= WIN, place - WIN, place)
        place_hot[i] = jnp.where(place_iota == place, 1.0, 0.0).astype(BF16)

    pooled_t = qz[z]
    for o in range(1, NZ):
        k = (z + o) % NZ
        remote(qz.at[k], zr.at[k], z_send.at[0], z_recv.at[k], left).wait_recv()
        pooled_t = pooled_t + zr[k]
    pooled = pooled_t.T

    v0 = bottom_ref[...].astype(F32)
    cot_in.wait()
    pairs_in.wait()
    pair_dots = jnp.sum(v0 * pooled, axis=1, keepdims=True)
    preact = pre_dense[...] + pair_dots * pairs_ref[...]
    gate = jax.nn.sigmoid(preact)
    pre_grad = cot_ref[...] * gate * (1.0 + preact * (1.0 - gate))
    pair_grad = jnp.sum(pre_grad * pairs_ref[...], axis=1, keepdims=True)
    pgs[chip] = jnp.broadcast_to(pair_grad, (B, B)).T[0:8]
    pg_out = [
        remote(pgs.at[chip], pgs.at[chip], pg_send.at[o - 1], pg_recv.at[chip], at((chip + o) % CHIPS))
        for o in range(1, CHIPS)
    ]
    for copy in pg_out:
        copy.start()
    act_ref[...] = (preact * gate).astype(BF16)
    bgrad_ref[...] = (
        lax.dot_general(
            pre_grad.astype(BF16), dense_ref[...], (((1,), (1,)), ((), ())), preferred_element_type=F32
        )
        + pair_grad * pooled
    )

    v_right.wait_recv()
    v_left.wait_recv()
    for o in range(1, NZ):
        k = (z + o) % NZ
        remote(vs.at[x_far, k], vs.at[x_far, k], far_send.at[0], far_recv.at[k], left).wait_recv()
    for o in range(1, CHIPS):
        k = (chip + o) % CHIPS
        remote(pgs.at[k], pgs.at[k], pg_send.at[o - 1], pg_recv.at[k], left).wait_recv()
    columns = pgs[...].reshape(CHIPS * 8, B).T
    for i in range(CHIPS):
        xi, zi = i // NZ, i % NZ
        q = zi // 2
        slot = q * 8 + 2 * turn_of(xi, q) + zi % 2
        high, low = split_bf16(vs[xi, zi] * columns[:, 8 * i : 8 * i + 1])
        grads[0, slot] = high
        grads[1, slot] = low

    parts = [(zh + 1 + z // 2) % ZH, (zh + 2 + 2 * (z // 2)) % ZH, zh]

    def row_grads(half, i):
        rows = [
            jnp.concatenate([et[k // 8][k % 8, half * (OWN // 256) + parts[i] * 2 + block] for k in range(CHIPS)], axis=1)
            for block in range(2)
        ]
        right_side = jnp.concatenate([grads[k].reshape(CHIPS * B, D) for k in range(2)], axis=1)
        both = jnp.dot(jnp.concatenate(rows, axis=0), right_side, preferred_element_type=F32)
        return both[:, 0:D] + both[:, D:]

    l_out = [remote(lsend.at[i], lrecv.at[i], l_send.at[i], l_recv.at[i], partner) for i in range(3)]
    g_out = []
    for i in range(3):
        lsend[i] = row_grads(1 - c, i)
        l_out[i].start()
        total = row_grads(c, i)
        l_out[i].wait_recv()
        outb[i] = (total + lrecv[i]).reshape(NY, HOT, D)
        for o in (0, 1, 7, 2, 6, 3, 5, 4):
            if i == 2 and o == 0:
                continue
            k = (y + o) % NY
            copy = remote(outb.at[i, k], grecv.at[g], g_send.at[len(g_out)], g_recv.at[g], (parts[i] * NY + k, s))
            copy.start()
            g_out.append(copy)
    grecv[g] = outb[2, y]
    for o in range(1, GROUPS):
        k = (g + o) % GROUPS
        remote(grecv.at[k], grecv.at[k], g_send.at[0], g_recv.at[k], left).wait_recv()
    high, low = split_bf16(grecv[...].reshape(OWN, D))
    both = jnp.dot(
        jnp.concatenate([place_hot[i] for i in range(OWN // B)], axis=1),
        jnp.concatenate([high, low], axis=1),
        preferred_element_type=F32,
    )
    tgrad_ref[...] = (both[:, 0:D] + both[:, D:])[0:WIN]

    hot_out.wait_send()
    for copy in (*idx_out, *vz_out, *rs_out.values(), v_right, v_left, far_out, *far_on):
        copy.wait_send()
    for copy in (*pg_out, *l_out, *g_out):
        copy.wait_send()
    for o in range(1, NZ):
        k = (z + o) % NZ
        remote(qz.at[k], zr.at[z], z_send.at[k], z_recv.at[z], at(x * NZ + k)).wait_send()


def keep(*refs):
    for source, target in zip(refs[:3], refs[3:]):
        target[...] = source[...]


def on_device(bottom_out, lookups, starts, tables, top_dense, top_pairs, cotangent):
    vmem = pl.BlockSpec(memory_space=pltpu.VMEM)
    dma = pltpu.SemaphoreType.DMA
    hbm = pl.BlockSpec(memory_space=pltpu.HBM)
    shapes = (
        jax.ShapeDtypeStruct((B, 1024), BF16),
        jax.ShapeDtypeStruct((B, D), F32),
        jax.ShapeDtypeStruct((WIN, D), F32),
    )
    operands = (
        bottom_out, lookups[:, 0, :].T, top_pairs, starts, tables.reshape(GROUPS, WIN, D), top_dense, cotangent,
    )
    results = pl.pallas_call(
        kernel,
        out_shape=shapes,
        in_specs=[hbm] * 7,
        out_specs=(vmem, vmem, vmem),
        scratch_shapes=[
            pltpu.VMEM((B, D), BF16),
            pltpu.VMEM((4, B), I32),
            pltpu.VMEM((1, 1024), F32),
            pltpu.VMEM((D, 1024), BF16),
            pltpu.VMEM((B, 1024), F32),
            pltpu.SMEM((GROUPS, 256), I32),
            pltpu.VMEM((GROUPS, PAD, D), F32),
            pltpu.VMEM((ROWS, D), F32),
            pltpu.VMEM((ROWS // 128, 2 * D, 128), BF16),
            pltpu.VMEM((CHIPS, 8, B), I32),
            pltpu.VMEM((CHIPS // 2, ROWS // 256, 256, B), BF16),
            pltpu.VMEM((CHIPS // 2, ROWS // 256, 256, B), BF16),
            pltpu.VMEM((8, 2, D, B), F32),
            pltpu.VMEM((6, 2, D, B), F32),
            pltpu.VMEM((NZ, D, B), F32),
            pltpu.VMEM((NZ, D, B), F32),
            pltpu.VMEM((NX, NZ, B, D), F32),
            pltpu.VMEM((CHIPS, 8, B), F32),
            pltpu.VMEM((2, CHIPS, B, D), BF16),
            pltpu.VMEM((B, 1024), F32),
            pltpu.VMEM((ZH, NY * HOT, D), F32),
            pltpu.VMEM((ZH, NY * HOT, D), F32),
            pltpu.VMEM((ZH, NY, HOT, D), F32),
            pltpu.VMEM((GROUPS, HOT, D), F32),
            pltpu.VMEM((OWN // B, OUT_ROWS, B), BF16),
            dma((8,)), dma((2,)), dma((CHIPS - 1,)), dma((CHIPS,)), dma((NZ - 1,)), dma((NZ,)), dma((NZ,)), dma((NZ,)), dma((2,)), dma((2,)),
            dma((6,)), dma((6,)), dma((NZ,)), dma((NZ,)), dma((CHIPS - 1,)), dma((CHIPS,)),
            dma((ZH,)), dma((ZH,)), dma((GROUPS,)), dma((GROUPS,)),
        ],
        compiler_params=pltpu.CompilerParams(
            collective_id=0, has_side_effects=True, vmem_limit_bytes=38 * 1024 * 1024
        ),
    )(
        *(pltpu.with_memory_space_constraint(value, pltpu.HBM) for value in operands)
    )
    act, bgrad, tgrad = pl.pallas_call(
        keep,
        out_shape=shapes,
        in_specs=[vmem] * 3,
        out_specs=(vmem,) * 3,
        compiler_params=pltpu.CompilerParams(vmem_limit_bytes=4 * 1024 * 1024),
    )(*results)
    return act, bgrad, tgrad[None, None]


def solution(mesh):
    in_specs = (
        P(("grp", "shard"), None),
        P(("grp", "shard"), None, None),
        P(),
        P(None, "shard", None),
        P(),
        P(),
        P(("grp", "shard"), None),
    )
    out_specs = (
        P(("grp", "shard"), None),
        P(("grp", "shard"), None),
        P(None, "shard", "grp", None),
    )
    return jax.shard_map(
        on_device, mesh=mesh, in_specs=in_specs, out_specs=out_specs, check_vma=False
    )
```
